128 devices in a mesh: rows: 32 (over x, z_hi, y), cols: 4 (over z_lo, core).
Axes of the slice: x: 4, y: 4, z: 4 (z_hi: 2, z_lo: 2; z = z_hi * 2 + z_lo), core: 2. Of those that a mesh axis runs over, the one named last changes fastest.
Arguments:
- mantissa: bfloat16 [8192, 8192], P('rows', 'cols'), may hold values from 0.5 to 1
- exponents: int32 [512, 64], P('rows'), may hold values from -3 to 1
Outputs:
- spectrum_real: float32 [8192, 8192], P(('rows', 'cols'))
- spectrum_imag: float32 [8192, 8192], P(('rows', 'cols'))
The draws below stay inside these ranges and needn't reach their ends.
Inputs may be any that keep to these rules, and one draw needn't show every extreme that they name: `exponents`: each entry scales its block of 16 rows and 128 columns of the table by 2 to that power.
All inputs are finite; a program needn't handle non-finite values.
Results may differ from the reference program's by a relative error of at most 0.0013.
Values may be sent and summed in bfloat16 or wider, within the bound.
A program may use at most 64 MiB of HBM per device.

```python
import math
import jax
import jax.numpy as jnp

NR = 8192
NC = 8192


def set_ends(result, key, low, largest):
    spot = [jax.random.randint(jax.random.fold_in(key, axis), (), 0, length) for axis, length in enumerate(result.shape)]
    main_axis = result.shape.index(max(result.shape))
    next_to = spot[:main_axis] + [(spot[main_axis] + 1) % result.shape[main_axis]] + spot[main_axis + 1:]
    return result.at[tuple(spot)].set(low).at[tuple(next_to)].set(largest)


def level_of(rng, shape, split, least, high):
    gain, own = 1.0, jax.random.fold_in(rng, 6)
    for axis_at, parts in split:
        heights = jnp.exp(jax.random.uniform(jax.random.fold_in(own, axis_at), (parts,), jnp.float32, least / len(split), high / len(split)))
        gain = gain * jnp.repeat(heights, shape[axis_at] // parts).reshape([-1 if axis == axis_at else 1 for axis in range(len(shape))])
    return gain


def setup_inputs(seed: int = 0) -> dict:
    keys = jax.random.split(jax.random.key(seed), 3)
    mantissa = jnp.clip(0.5 + 0.5 * jax.random.uniform(keys[0], (NR, NC), jnp.float32) ** level_of(keys[0], (NR, NC), ((0, 32), (1, 4)), -0.2, 0.2), 0.5, 1.0).astype(jnp.bfloat16)
    exponents = set_ends(jax.random.randint(keys[1], (NR // 16, NC // 128), -3, 2), jax.random.fold_in(keys[1], 1), -3, 1).astype(jnp.int32)
    return dict(mantissa=mantissa, exponents=exponents)


def reference(mantissa, exponents):
    scaling = jnp.exp2(exponents.astype(jnp.float32))
    cumulative = (mantissa.astype(jnp.float32).reshape(NR // 16, 16, NC // 128, 128) * scaling[:, None, :, None]).reshape(NR, NC)
    padded = jnp.pad(cumulative, ((1, 0), (1, 0)))
    masses = cumulative - padded[:-1, 1:] - (padded[1:, :-1] - padded[:-1, :-1])
    spectrum = jnp.fft.fft2(masses) / math.sqrt(NR * NC)
    return (jnp.real(spectrum).T.astype(jnp.float32), jnp.imag(spectrum).T.astype(jnp.float32))
```

```python
import math

import jax
import jax.numpy as jnp
import ml_dtypes
import numpy as np
from jax import lax
from jax.experimental import pallas as pl
from jax.experimental.pallas import tpu as pltpu
from jax.sharding import PartitionSpec as P

NR = 8192
NC = 8192
MESH = pl.DeviceIdType.MESH
CHUNKS = 8
LAG = 2
TOP = 32767.0
BOUND = 16896.0
F32 = jnp.float32
BF16 = jnp.bfloat16


def halves(table):
    high = table.astype(ml_dtypes.bfloat16)
    low = (table - high.astype(np.float64)).astype(ml_dtypes.bfloat16)
    return np.stack([high, low])


def send_table():
    sides = []
    for side in range(2):
        t = np.arange(64)
        row, core = t // 2, t % 2
        z_lo = ((row // 4) % 2 + side) % 2
        a = 4 * row + 2 * z_lo + core
        jo = np.arange(128)[:, None]
        one = 2 * np.pi * (jo * a % 128) / 128
        two = 2 * np.pi * (jo * (a + 1) % 128) / 128
        from_re = np.concatenate([np.cos(one), -np.sin(one), np.cos(two), -np.sin(two)], 1)
        from_im = np.concatenate([np.sin(one), np.cos(one), -np.sin(two), -np.cos(two)], 1)
        sides.append(halves(np.concatenate([from_re, from_im], 0)))
    return np.stack(sides)


def receive_table():
    k0 = np.arange(128)[None, :]
    blocks = []
    for half in range(2):
        s = 2 * np.arange(64)[:, None] + half
        angle = 2 * np.pi * (s * k0 % 128) / 128
        blocks.append(np.concatenate([np.cos(angle), -np.sin(angle)], 1))
        blocks.append(np.concatenate([np.sin(angle), np.cos(angle)], 1))
    return halves(np.concatenate(blocks, 0))


def twist_table(count, scale):
    angle = 2 * np.pi * (np.arange(count)[:, None] * np.arange(128)[None, :]) / 8192
    table = np.stack([np.cos(angle), -np.sin(angle)], 1).reshape(2 * count, 128) * scale
    return table.astype(np.float32)


def c_add(u, v):
    im = v[1] if u[1] is None else (u[1] if v[1] is None else u[1] + v[1])
    return (u[0] + v[0], im)


def c_sub(u, v):
    im = (None if v[1] is None else -v[1]) if u[1] is None else (u[1] if v[1] is None else u[1] - v[1])
    return (u[0] - v[0], im)


def sub_i(u, v):
    re = u[0] if v[1] is None else u[0] + v[1]
    return (re, -v[0] if u[1] is None else u[1] - v[0])


def add_i(u, v):
    re = u[0] if v[1] is None else u[0] - v[1]
    return (re, v[0] if u[1] is None else u[1] + v[0])


def c_scale(u, cos, sin):
    if u[1] is None:
        return (u[0] * cos, u[0] * (-sin))
    return (u[0] * cos + u[1] * sin, u[1] * cos - u[0] * sin)


ROOT = math.sqrt(0.5)


def dft4(x):
    t0, t1 = c_add(x[0], x[2]), c_sub(x[0], x[2])
    t2, t3 = c_add(x[1], x[3]), c_sub(x[1], x[3])
    return [c_add(t0, t2), sub_i(t1, t3), c_sub(t0, t2), add_i(t1, t3)]


def dft8(x, half=False):
    even, odd = dft4(x[0::2]), dft4(x[1::2])
    o1, o3 = odd[1], odd[3]
    w1 = ((o1[0] + o1[1]) * ROOT, (o1[1] - o1[0]) * ROOT)
    y = [c_add(even[0], odd[0]), c_add(even[1], w1), sub_i(even[2], odd[2]), None, c_sub(even[0], odd[0])]
    w3 = ((o3[1] - o3[0]) * ROOT, (o3[0] + o3[1]) * -ROOT)
    y[3] = c_add(even[3], w3)
    if half:
        return y
    return y + [c_sub(even[1], w1), add_i(even[2], odd[2]), c_sub(even[3], w3)]


def twist64(u, n):
    n = n % 64
    if n == 0:
        return u
    return c_scale(u, math.cos(2 * math.pi * n / 64), math.sin(2 * math.pi * n / 64))


def code(x):
    u = lax.rsqrt(lax.rsqrt(jnp.maximum(jnp.abs(x) * (1.0 / BOUND), 1e-30)))
    n = (u * TOP + 0.5).astype(jnp.int32)
    return jnp.where(x < 0, -n, n)


def decode(n):
    v = n.astype(F32)
    return (v * jnp.abs(v)) * (v * v)


DECODED = BOUND / TOP**4


def split(x):
    high = x.astype(BF16)
    return high, (x - high.astype(F32)).astype(BF16)


def exchange(
    mant, exps_in, send_w, recv_w, send_t, recv_t,
    z_out,
    block, masses, first, a_hi, a_lo, products, words, outbox, inbox, b_hi, b_lo, result,
    exps, w_ref, e_ref, t1_ref, t2_ref, edge_in, edge, above, last, last_in,
    s_blk, r_blk, s_out, r_out, s_edge, r_edge, s_last, r_last, tab_sem, edge_sem, z_sem, exp_sem, sem_b, sem_c, sem_d,
):
    row, col = lax.axis_index("rows"), lax.axis_index("cols")
    x, z_hi, y = row // 8, (row // 4) % 2, row % 4
    z_lo, core = col // 2, col % 2
    side = (z_hi + z_lo) % 2
    me = row * 2 + core
    my_cols = pl.ds(pl.multiple_of(2048 * col, 2048), 2048)

    def at(r, c):
        return dict(device_id={"rows": r, "cols": c}, device_id_type=MESH)

    def mate(m):
        other = (core + m % 2) % 2
        return ((z_lo + m // 2) % 2) * 2 + other, other

    tables = (
        pltpu.make_async_copy(send_w.at[side], w_ref, tab_sem.at[0]),
        pltpu.make_async_copy(recv_w, e_ref, tab_sem.at[1]),
        pltpu.make_async_copy(send_t, t1_ref, tab_sem.at[2]),
        pltpu.make_async_copy(recv_t, t2_ref, tab_sem.at[3]),
    )
    edges = (
        pltpu.make_async_copy(mant.at[:, 0], edge_in.at[0], edge_sem.at[0]),
        pltpu.make_async_copy(mant.at[:, 7], edge_in.at[1], edge_sem.at[1]),
    )
    exp_copy = pltpu.make_async_copy(exps_in, exps, exp_sem)
    exp_copy.start()
    for copy in edges + tables:
        copy.start()

    barrier = pltpu.get_barrier_semaphore()
    count = 0
    for m in (1, 2, 3):
        pl.semaphore_signal(barrier, inc=1, **at(row, mate(m)[0]))
        count += 1
    for other in (core, 1 - core):
        pl.semaphore_signal(barrier, inc=1, **at(x * 8 + (1 - z_hi) * 4 + y, (1 - z_lo) * 2 + other))
        count += 1
    for d in (1, 2, 3):
        pl.semaphore_signal(barrier, inc=1, **at(x * 8 + z_hi * 4 + (y + d) % 4, col))
        pl.semaphore_signal(barrier, inc=1, **at((x + d) % 4 * 8 + z_hi * 4 + y, col))
        count += 2

    exp_copy.wait()
    for copy in edges:
        copy.wait()
    for g in range(4):
        for j in range(16):
            lanes = slice(128 * j, 128 * (j + 1))
            e = exps[4 * g, 16 * col + j]
            scale = jnp.left_shift(1, e + 3).astype(F32) * 0.125
            edge[g // 2, g % 2 : g % 2 + 1, lanes] = edge_in[0, g, :, lanes].astype(F32)[7:8] * scale
            if g % 2:
                e = exps[4 * g + 3, 16 * col + j]
                scale = jnp.left_shift(1, e + 3).astype(F32) * 0.125
                last[g // 2, :, lanes] = edge_in[1, g, :, lanes].astype(F32)[7:8] * scale

    pl.semaphore_wait(barrier, count)
    for m in (1, 2, 3):
        c, other = mate(m)
        pltpu.make_async_remote_copy(
            edge.at[other], above.at[:, my_cols], s_edge, r_edge, **at(row, c)
        ).start()
    pltpu.make_async_copy(edge.at[core], above.at[:, my_cols], r_edge).start()

    def send_block(q):
        for m in (2, 3, 1):
            c, other = mate(m)
            pltpu.make_async_remote_copy(
                mant.at[pl.ds(2 * other, 2), q], block.at[:, q, :, my_cols], s_blk.at[q], r_blk.at[q], **at(row, c)
            ).start()
        pltpu.make_async_copy(
            mant.at[pl.ds(2 * core, 2), q], block.at[:, q, :, my_cols], r_blk.at[q]
        ).start()

    @pl.loop(0, CHUNKS)
    def _(j):
        send_block((j + 1) % CHUNKS)

    for d in (1, 2, 3):
        pl.semaphore_signal(sem_b, inc=1, **at(x * 8 + z_hi * 4 + (y + d) % 4, col))
    pl.semaphore_wait(sem_b, 3)
    for d in (1, 2, 3):
        pl.semaphore_signal(sem_c, inc=1, **at((x + d) % 4 * 8 + z_hi * 4 + y, col))

    for copy in tables:
        copy.wait()
    ref = above
    pltpu.make_async_copy(ref, ref, r_edge).wait()
    sub8 = lax.broadcasted_iota(jnp.int32, (8, 128), 0)
    lane8 = lax.broadcasted_iota(jnp.int32, (8, 128), 1)

    pl.semaphore_wait(sem_c, 3)
    pl.semaphore_signal(sem_d, inc=1, **at(x * 8 + (1 - z_hi) * 4 + y, (1 - z_lo) * 2 + core))

    def send_last():
        pl.semaphore_wait(sem_d, 1)
        for m in (1, 2, 3):
            c, other = mate(m)
            pltpu.make_async_remote_copy(
                last.at[1 - other], last_in.at[:, my_cols], s_last, r_last, **at((row + 1 - other) % 32, c)
            ).start()

        @pl.when(core == 1)
        def _():
            pltpu.make_async_copy(last.at[0], last_in.at[:, my_cols], r_last).start()

        @pl.when(core == 0)
        def _():
            pltpu.make_async_remote_copy(
                last.at[1], last_in.at[:, my_cols], s_last, r_last, **at((row + 1) % 32, col)
            ).start()

    def send_phase(q):
        ref = block.at[:, q]
        pltpu.make_async_copy(ref, ref, r_blk.at[q]).wait()

        for h in range(2):
            before = None
            for c in range(64):
                lanes = slice(128 * c, 128 * (c + 1))
                e = exps[8 * core + 4 * h + q // 2, c]
                scale = jnp.left_shift(1, e + 3).astype(F32) * 0.125
                here = block[h, q, :, lanes].astype(F32) * scale
                top = jnp.broadcast_to(above[h : h + 1, lanes], (8, 128))
                upper = jnp.where(sub8 == 0, top, pltpu.roll(here, 1, 0))
                above[h : h + 1, lanes] = here[7:8]
                step = here - upper
                rolled = pltpu.roll(step, 1, 1)
                left = jnp.where(lane8 == 0, 0.0 if before is None else before, rolled)
                before = rolled
                masses[c, 8 * h : 8 * h + 8, :] = step - left

        for c0 in range(8):
            spread = dft8([(masses[8 * c1 + c0], None) for c1 in range(8)], half=True)
            for b1 in range(5):
                value = twist64(spread[b1], c0 * b1)
                first[b1, c0, 0] = value[0]
                if value[1] is not None:
                    first[b1, c0, 1] = value[1]
        for b1 in range(5):
            real = b1 == 0
            spread = dft8(
                [
                    (first[b1, c0, 0], None if real or (b1 == 4 and c0 == 0) else first[b1, c0, 1])
                    for c0 in range(8)
                ],
                half=real,
            )
            for b0, (re, im) in enumerate(spread):
                b = b1 + 8 * b0
                if b1 == 4 and b0 >= 4:
                    continue
                if b > 32:
                    b, im = 64 - b, -im
                if b == 0:
                    tw_re, tw_im = re, jnp.zeros_like(re)
                else:
                    cos = jnp.broadcast_to(t1_ref[2 * b : 2 * b + 1, :], (16, 128))
                    sin = jnp.broadcast_to(t1_ref[2 * b + 1 : 2 * b + 2, :], (16, 128))
                    if im is None:
                        tw_re, tw_im = re * cos, re * sin
                    else:
                        tw_re, tw_im = re * cos - im * sin, re * sin + im * cos
                rows = slice(16 * b, 16 * b + 16)
                a_hi[rows, 0:128], a_lo[rows, 0:128] = split(tw_re)
                a_hi[rows, 128:256], a_lo[rows, 128:256] = split(tw_im)

        high = a_hi[...]
        products[...] = (
            jnp.dot(high, w_ref[0], preferred_element_type=F32)
            + jnp.dot(a_lo[...], w_ref[0], preferred_element_type=F32)
            + jnp.dot(high, w_ref[1], preferred_element_type=F32)
        )

        for b in range(33):
            for place, lanes in ((b, slice(0, 128)), (64 - b, slice(128, 256))):
                if b in (0, 32) and lanes.start:
                    continue
                low = code(products[16 * b : 16 * b + 8, lanes])
                top = code(products[16 * b + 8 : 16 * b + 16, lanes])
                words[8 * place : 8 * place + 8, :] = jnp.left_shift(top, 16) | (low & 0xFFFF)
        for p in range(4):
            tile = jnp.concatenate(
                [words[pl.ds(64 * g + i, 8, stride=8), :] for i in (2 * p, 2 * p + 1) for g in range(8)], 0
            )
            lanes = pl.ds(pl.multiple_of(512 * q + 128 * p, 128), 128)
            outbox[:, :, lanes] = tile.T.reshape(2, 64, 128)

        lanes = pl.ds(pl.multiple_of(512 * q, 512), 512)

        @pl.loop(1, 64)
        def _(m):
            flip, dc, dx, dy = m % 2, (m // 32) % 2, (m // 2) % 4, (m // 8) % 4
            to_hi, to_lo, to_core = (z_hi + flip) % 2, (z_lo + flip) % 2, (core + dc) % 2
            to_row = (x + dx) % 4 * 8 + to_hi * 4 + (y + dy) % 4
            pltpu.make_async_remote_copy(
                outbox.at[:, pl.ds(to_row * 2 + to_core, 1), lanes],
                inbox.at[:, pl.ds(me, 1), lanes],
                s_out.at[q],
                r_out.at[q],
                **at(to_row, to_lo * 2 + to_core),
            ).start()

        pltpu.make_async_copy(
            outbox.at[:, pl.ds(me, 1), lanes], inbox.at[:, pl.ds(me, 1), lanes], r_out.at[q]
        ).start()

    def receive_phase(q):
        lanes = pl.ds(pl.multiple_of(512 * q, 512), 512)
        ref = inbox.at[:, :, lanes]
        pltpu.make_async_copy(ref, ref, r_out.at[q]).wait()
        for p in range(4):
            lanes = pl.ds(pl.multiple_of(512 * q + 128 * p, 128), 128)
            tile = inbox[:, :, lanes].reshape(128, 128).T
            rows = slice(128 * p, 128 * p + 128)
            low = decode(jnp.right_shift(jnp.left_shift(tile, 16), 16))
            b_hi[rows, 0:128], b_lo[rows, 0:128] = split(low)
            top = decode(jnp.right_shift(tile, 16))
            b_hi[rows, 128:256], b_lo[rows, 128:256] = split(top)
        high = b_hi[...]
        value = (
            jnp.dot(high, e_ref[0], preferred_element_type=F32)
            + jnp.dot(b_lo[...], e_ref[0], preferred_element_type=F32)
            + jnp.dot(high, e_ref[1], preferred_element_type=F32)
        )
        for i in range(8):
            re, im = value[64 * i : 64 * i + 64, 0:128], value[64 * i : 64 * i + 64, 128:256]
            cos = t2_ref[pl.ds(16 * q + 2 * i, 1), :]
            sin = t2_ref[pl.ds(16 * q + 2 * i + 1, 1), :]
            result[8 * q + i, :, 0:128] = re * cos - im * sin
            result[8 * q + i, :, 128:256] = re * sin + im * cos
        ref = pl.ds(8 * q, 8)
        pltpu.make_async_copy(result.at[ref], z_out.at[ref], z_sem.at[q]).start()

    @pl.loop(0, CHUNKS + LAG)
    def _(j):
        @pl.when(j == CHUNKS - 1)
        def _():
            pltpu.make_async_copy(last_in, last_in, r_last).wait()
            above[1:2, :] = above[0:1, :]
            above[0:1, :] = jnp.where(row * 2 + core == 0, jnp.zeros_like(last_in[...]), last_in[...])

        @pl.when(j == 2)
        def _():
            send_last()

        @pl.when(j < CHUNKS)
        def _():
            send_phase((j + 1) % CHUNKS)

        @pl.when(j >= LAG)
        def _():
            receive_phase((j - LAG + 1) % CHUNKS)

    for m in (1, 2, 3):
        pltpu.make_async_copy(edge.at[0], edge.at[0], s_edge).wait()
    for q in range(CHUNKS):
        ref = block.at[:, q, :, pl.ds(0, 6144)]
        pltpu.make_async_copy(ref, ref, s_blk.at[q]).wait()
        ref = outbox.at[0, pl.ds(0, 24), pl.ds(0, 2688)]
        pltpu.make_async_copy(ref, ref, s_out.at[q]).wait()
        ref = pl.ds(8 * q, 8)
        pltpu.make_async_copy(result.at[ref], z_out.at[ref], z_sem.at[q]).wait()
    for m in (1, 2, 3):
        pltpu.make_async_copy(last.at[0], last.at[0], s_last).wait()

    @pl.when(core == 0)
    def _():
        pltpu.make_async_copy(last.at[0], last.at[0], s_last).wait()


def run_exchange(mantissa, exponents):
    dma = pltpu.SemaphoreType.DMA
    operands = (
        mantissa.reshape(4, 8, 8, 2048),
        exponents,
        jnp.asarray(send_table()),
        jnp.asarray(receive_table()),
        jnp.asarray(np.concatenate([twist_table(33, 1.0), np.zeros((6, 128), np.float32)])),
        jnp.asarray(twist_table(64, DECODED / math.sqrt(NR * NC))),
    )
    return pl.pallas_call(
        exchange,
        out_shape=jax.ShapeDtypeStruct((64, 64, 256), F32),
        in_specs=[pl.BlockSpec(memory_space=pltpu.HBM)] * 6,
        out_specs=pl.BlockSpec(memory_space=pl.ANY),
        scratch_shapes=[
            pltpu.VMEM((2, 8, 8, 8192), BF16),
            pltpu.VMEM((64, 16, 128), F32),
            pltpu.VMEM((5, 8, 2, 16, 128), F32),
            pltpu.VMEM((528, 256), BF16),
            pltpu.VMEM((528, 256), BF16),
            pltpu.VMEM((528, 256), F32),
            pltpu.VMEM((512, 128), jnp.int32),
            pltpu.VMEM((2, 64, 4096), jnp.int32),
            pltpu.VMEM((2, 64, 4096), jnp.int32),
            pltpu.VMEM((512, 256), BF16),
            pltpu.VMEM((512, 256), BF16),
            pltpu.VMEM((64, 64, 256), F32),
            pltpu.SMEM((16, 64), jnp.int32),
            pltpu.VMEM((2, 256, 256), BF16),
            pltpu.VMEM((2, 256, 256), BF16),
            pltpu.VMEM((72, 128), F32),
            pltpu.VMEM((128, 128), F32),
            pltpu.VMEM((2, 4, 8, 2048), BF16),
            pltpu.VMEM((2, 2, 2048), F32),
            pltpu.VMEM((2, 8192), F32),
            pltpu.VMEM((2, 1, 2048), F32),
            pltpu.VMEM((1, 8192), F32),
            dma((CHUNKS,)),
            dma((CHUNKS,)),
            dma((CHUNKS,)),
            dma((CHUNKS,)),
            dma,
            dma,
            dma,
            dma,
            dma((4,)),
            dma((2,)),
            dma((CHUNKS,)),
            dma,
            pltpu.SemaphoreType.REGULAR,
            pltpu.SemaphoreType.REGULAR,
            pltpu.SemaphoreType.REGULAR,
        ],
        compiler_params=pltpu.CompilerParams(
            collective_id=0, has_side_effects=True, vmem_limit_bytes=48 * 1024 * 1024
        ),
        name="exchange",
    )(*[pltpu.with_memory_space_constraint(operand, pltpu.HBM) for operand in operands])


def finish(z_ref, re_ref, im_ref, middle):
    for i0 in range(8):
        spread = dft8([(z_ref[8 * i1 + i0, :, 0:128], z_ref[8 * i1 + i0, :, 128:256]) for i1 in range(8)])
        for k_a in range(8):
            value = twist64(spread[k_a], i0 * k_a)
            middle[k_a, i0, 0] = value[0]
            middle[k_a, i0, 1] = value[1]
    for k_a in range(8):
        spread = dft8([(middle[k_a, i0, 0], middle[k_a, i0, 1]) for i0 in range(8)])
        for k_b, (re, im) in enumerate(spread):
            lanes = slice(128 * (k_a + 8 * k_b), 128 * (k_a + 8 * k_b + 1))
            re_ref[:, lanes] = re
            im_ref[:, lanes] = im


def run_finish(z):
    return pl.pallas_call(
        finish,
        grid=(8,),
        out_shape=[jax.ShapeDtypeStruct((64, NR), F32)] * 2,
        in_specs=[pl.BlockSpec((64, 8, 256), lambda g: (0, g, 0))],
        out_specs=[pl.BlockSpec((8, NR), lambda g: (g, 0))] * 2,
        scratch_shapes=[pltpu.VMEM((8, 8, 2, 8, 128), F32)],
        compiler_params=pltpu.CompilerParams(vmem_limit_bytes=48 * 1024 * 1024),
        name="finish",
    )(z)


def local(mantissa, exponents):
    re, im = run_finish(run_exchange(mantissa, exponents))
    return re, im


def solution(mesh):
    in_specs = (P("rows", "cols"), P("rows", None))
    out_specs = (P(("rows", "cols"), None), P(("rows", "cols"), None))
    return jax.shard_map(local, mesh=mesh, in_specs=in_specs, out_specs=out_specs, check_vma=False)
```

```python
import math

import jax
import jax.numpy as jnp
import ml_dtypes
import numpy as np
from jax import lax
from jax.experimental import pallas as pl
from jax.experimental.pallas import tpu as pltpu
from jax.sharding import PartitionSpec as P

NR = 8192
NC = 8192
MESH = pl.DeviceIdType.MESH
CHUNKS = 8
LAG = 2
TOP = 32767.0
BOUND = 16896.0
F32 = jnp.float32
BF16 = jnp.bfloat16


def halves(table):
    high = table.astype(ml_dtypes.bfloat16)
    low = (table - high.astype(np.float64)).astype(ml_dtypes.bfloat16)
    return np.stack([high, low])


def send_table():
    sides = []
    for side in range(2):
        t = np.arange(64)
        row, core = t // 2, t % 2
        z_lo = ((row // 4) % 2 + side) % 2
        a = 4 * row + 2 * z_lo + core
        jo = np.arange(128)[:, None]
        one = 2 * np.pi * (jo * a % 128) / 128
        two = 2 * np.pi * (jo * (a + 1) % 128) / 128
        from_re = np.concatenate([np.cos(one), -np.sin(one), np.cos(two), -np.sin(two)], 1)
        from_im = np.concatenate([np.sin(one), np.cos(one), -np.sin(two), -np.cos(two)], 1)
        sides.append(halves(np.concatenate([from_re, from_im], 0)))
    return np.stack(sides)


def receive_table():
    k0 = np.arange(128)[None, :]
    blocks = []
    for half in range(2):
        s = 2 * np.arange(64)[:, None] + half
        angle = 2 * np.pi * (s * k0 % 128) / 128
        blocks.append(np.concatenate([np.cos(angle), -np.sin(angle)], 1))
        blocks.append(np.concatenate([np.sin(angle), np.cos(angle)], 1))
    return halves(np.concatenate(blocks, 0))


def twist_table(count, scale):
    angle = 2 * np.pi * (np.arange(count)[:, None] * np.arange(128)[None, :]) / 8192
    table = np.stack([np.cos(angle), -np.sin(angle)], 1).reshape(2 * count, 128) * scale
    return table.astype(np.float32)


def c_add(u, v):
    im = v[1] if u[1] is None else (u[1] if v[1] is None else u[1] + v[1])
    return (u[0] + v[0], im)


def c_sub(u, v):
    im = (None if v[1] is None else -v[1]) if u[1] is None else (u[1] if v[1] is None else u[1] - v[1])
    return (u[0] - v[0], im)


def sub_i(u, v):
    re = u[0] if v[1] is None else u[0] + v[1]
    return (re, -v[0] if u[1] is None else u[1] - v[0])


def add_i(u, v):
    re = u[0] if v[1] is None else u[0] - v[1]
    return (re, v[0] if u[1] is None else u[1] + v[0])


def c_scale(u, cos, sin):
    if u[1] is None:
        return (u[0] * cos, u[0] * (-sin))
    return (u[0] * cos + u[1] * sin, u[1] * cos - u[0] * sin)


ROOT = math.sqrt(0.5)


def dft4(x):
    t0, t1 = c_add(x[0], x[2]), c_sub(x[0], x[2])
    t2, t3 = c_add(x[1], x[3]), c_sub(x[1], x[3])
    return [c_add(t0, t2), sub_i(t1, t3), c_sub(t0, t2), add_i(t1, t3)]


def dft8(x, half=False):
    even, odd = dft4(x[0::2]), dft4(x[1::2])
    o1, o3 = odd[1], odd[3]
    w1 = ((o1[0] + o1[1]) * ROOT, (o1[1] - o1[0]) * ROOT)
    y = [c_add(even[0], odd[0]), c_add(even[1], w1), sub_i(even[2], odd[2]), None, c_sub(even[0], odd[0])]
    w3 = ((o3[1] - o3[0]) * ROOT, (o3[0] + o3[1]) * -ROOT)
    y[3] = c_add(even[3], w3)
    if half:
        return y
    return y + [c_sub(even[1], w1), add_i(even[2], odd[2]), c_sub(even[3], w3)]


def twist64(u, n):
    n = n % 64
    if n == 0:
        return u
    return c_scale(u, math.cos(2 * math.pi * n / 64), math.sin(2 * math.pi * n / 64))


def code(x):
    u = lax.rsqrt(lax.rsqrt(jnp.maximum(jnp.abs(x) * (1.0 / BOUND), 1e-30)))
    n = (u * TOP + 0.5).astype(jnp.int32)
    return jnp.where(x < 0, -n, n)


def decode(n):
    v = n.astype(F32)
    return (v * jnp.abs(v)) * (v * v)


DECODED = BOUND / TOP**4


def split(x):
    high = x.astype(BF16)
    return high, (x - high.astype(F32)).astype(BF16)


def exchange(
    mant, exps_in, send_w, recv_w, send_t, recv_t,
    z_out,
    block, masses, first, a_hi, a_lo, products, words, outbox, inbox, b_hi, b_lo, result,
    exps, w_ref, e_ref, t1_ref, t2_ref, edge_in, edge, above, last, last_in,
    s_blk, r_blk, s_out, r_out, s_edge, r_edge, s_last, r_last, tab_sem, edge_sem, z_sem, exp_sem, sem_b, sem_c, sem_d,
):
    row, col = lax.axis_index("rows"), lax.axis_index("cols")
    x, z_hi, y = row // 8, (row // 4) % 2, row % 4
    z_lo, core = col // 2, col % 2
    side = (z_hi + z_lo) % 2
    me = row * 2 + core
    my_cols = pl.ds(pl.multiple_of(2048 * col, 2048), 2048)

    def at(r, c):
        return dict(device_id={"rows": r, "cols": c}, device_id_type=MESH)

    def mate(m):
        other = (core + m % 2) % 2
        return ((z_lo + m // 2) % 2) * 2 + other, other

    tables = (
        pltpu.make_async_copy(send_w.at[side], w_ref, tab_sem.at[0]),
        pltpu.make_async_copy(recv_w, e_ref, tab_sem.at[1]),
        pltpu.make_async_copy(send_t, t1_ref, tab_sem.at[2]),
        pltpu.make_async_copy(recv_t, t2_ref, tab_sem.at[3]),
    )
    edges = (
        pltpu.make_async_copy(mant.at[:, 0], edge_in.at[0], edge_sem.at[0]),
        pltpu.make_async_copy(mant.at[:, 7], edge_in.at[1], edge_sem.at[1]),
    )
    exp_copy = pltpu.make_async_copy(exps_in, exps, exp_sem)
    exp_copy.start()
    for copy in edges + tables:
        copy.start()

    barrier = pltpu.get_barrier_semaphore()
    count = 0
    for m in (1, 2, 3):
        pl.semaphore_signal(barrier, inc=1, **at(row, mate(m)[0]))
        count += 1
    for other in (core, 1 - core):
        pl.semaphore_signal(barrier, inc=1, **at(x * 8 + (1 - z_hi) * 4 + y, (1 - z_lo) * 2 + other))
        count += 1
    for d in (1, 2, 3):
        pl.semaphore_signal(barrier, inc=1, **at(x * 8 + z_hi * 4 + (y + d) % 4, col))
        pl.semaphore_signal(barrier, inc=1, **at((x + d) % 4 * 8 + z_hi * 4 + y, col))
        count += 2

    exp_copy.wait()
    for copy in edges:
        copy.wait()
    for g in range(4):
        for j in range(16):
            lanes = slice(128 * j, 128 * (j + 1))
            e = exps[4 * g, 16 * col + j]
            scale = jnp.left_shift(1, e + 3).astype(F32) * 0.125
            edge[g // 2, g % 2 : g % 2 + 1, lanes] = edge_in[0, g, :, lanes].astype(F32)[7:8] * scale
            if g % 2:
                e = exps[4 * g + 3, 16 * col + j]
                scale = jnp.left_shift(1, e + 3).astype(F32) * 0.125
                last[g // 2, :, lanes] = edge_in[1, g, :, lanes].astype(F32)[7:8] * scale

    pl.semaphore_wait(barrier, count)
    for m in (1, 2, 3):
        c, other = mate(m)
        pltpu.make_async_remote_copy(
            edge.at[other], above.at[:, my_cols], s_edge, r_edge, **at(row, c)
        ).start()
    pltpu.make_async_copy(edge.at[core], above.at[:, my_cols], r_edge).start()

    def send_block(q):
        for m in (2, 3, 1):
            c, other = mate(m)
            pltpu.make_async_remote_copy(
                mant.at[pl.ds(2 * other, 2), q], block.at[:, q, :, my_cols], s_blk.at[q], r_blk.at[q], **at(row, c)
            ).start()
        pltpu.make_async_copy(
            mant.at[pl.ds(2 * core, 2), q], block.at[:, q, :, my_cols], r_blk.at[q]
        ).start()

    @pl.loop(0, CHUNKS)
    def _(j):
        send_block((j + 1) % CHUNKS)

    for d in (1, 2, 3):
        pl.semaphore_signal(sem_b, inc=1, **at(x * 8 + z_hi * 4 + (y + d) % 4, col))
    pl.semaphore_wait(sem_b, 3)
    for d in (1, 2, 3):
        pl.semaphore_signal(sem_c, inc=1, **at((x + d) % 4 * 8 + z_hi * 4 + y, col))

    for copy in tables:
        copy.wait()
    ref = above
    pltpu.make_async_copy(ref, ref, r_edge).wait()
    sub8 = lax.broadcasted_iota(jnp.int32, (8, 128), 0)
    lane8 = lax.broadcasted_iota(jnp.int32, (8, 128), 1)

    pl.semaphore_wait(sem_c, 3)
    pl.semaphore_signal(sem_d, inc=1, **at(x * 8 + (1 - z_hi) * 4 + y, (1 - z_lo) * 2 + core))

    def send_last():
        pl.semaphore_wait(sem_d, 1)
        for m in (1, 2, 3):
            c, other = mate(m)
            pltpu.make_async_remote_copy(
                last.at[1 - other], last_in.at[:, my_cols], s_last, r_last, **at((row + 1 - other) % 32, c)
            ).start()

        @pl.when(core == 1)
        def _():
            pltpu.make_async_copy(last.at[0], last_in.at[:, my_cols], r_last).start()

        @pl.when(core == 0)
        def _():
            pltpu.make_async_remote_copy(
                last.at[1], last_in.at[:, my_cols], s_last, r_last, **at((row + 1) % 32, col)
            ).start()

    def wrap4(n):
        return jnp.where(n >= 4, n - 4, n)

    to_y = [wrap4(y + d) for d in range(4)]
    corners = []
    for flip in range(2):
        for d in range(2):
            to_hi = 1 - z_hi if flip else z_hi
            to_lo = 1 - z_lo if flip else z_lo
            to_core = 1 - core if d else core
            corners.append((to_hi * 8 + to_core, to_hi * 4, to_lo * 2 + to_core))

    def send_phase(q):
        ref = block.at[:, q]
        pltpu.make_async_copy(ref, ref, r_blk.at[q]).wait()

        for h in range(2):
            before = None
            for c in range(64):
                lanes = slice(128 * c, 128 * (c + 1))
                e = exps[8 * core + 4 * h + q // 2, c]
                scale = jnp.left_shift(1, e + 3).astype(F32) * 0.125
                here = block[h, q, :, lanes].astype(F32) * scale
                top = jnp.broadcast_to(above[h : h + 1, lanes], (8, 128))
                upper = jnp.where(sub8 == 0, top, pltpu.roll(here, 1, 0))
                above[h : h + 1, lanes] = here[7:8]
                step = here - upper
                rolled = pltpu.roll(step, 1, 1)
                left = jnp.where(lane8 == 0, 0.0 if before is None else before, rolled)
                before = rolled
                masses[c, 8 * h : 8 * h + 8, :] = step - left

        for c0 in range(8):
            spread = dft8([(masses[8 * c1 + c0], None) for c1 in range(8)], half=True)
            for b1 in range(5):
                value = twist64(spread[b1], c0 * b1)
                first[b1, c0, 0] = value[0]
                if value[1] is not None:
                    first[b1, c0, 1] = value[1]
        for b1 in range(5):
            real = b1 == 0
            spread = dft8(
                [
                    (first[b1, c0, 0], None if real or (b1 == 4 and c0 == 0) else first[b1, c0, 1])
                    for c0 in range(8)
                ],
                half=real,
            )
            for b0, (re, im) in enumerate(spread):
                b = b1 + 8 * b0
                if b1 == 4 and b0 >= 4:
                    continue
                if b > 32:
                    b, im = 64 - b, -im
                if b == 0:
                    tw_re, tw_im = re, jnp.zeros_like(re)
                else:
                    cos = jnp.broadcast_to(t1_ref[2 * b : 2 * b + 1, :], (16, 128))
                    sin = jnp.broadcast_to(t1_ref[2 * b + 1 : 2 * b + 2, :], (16, 128))
                    if im is None:
                        tw_re, tw_im = re * cos, re * sin
                    else:
                        tw_re, tw_im = re * cos - im * sin, re * sin + im * cos
                rows = slice(16 * b, 16 * b + 16)
                a_hi[rows, 0:128], a_lo[rows, 0:128] = split(tw_re)
                a_hi[rows, 128:256], a_lo[rows, 128:256] = split(tw_im)

        high = a_hi[...]
        products[...] = (
            jnp.dot(high, w_ref[0], preferred_element_type=F32)
            + jnp.dot(a_lo[...], w_ref[0], preferred_element_type=F32)
            + jnp.dot(high, w_ref[1], preferred_element_type=F32)
        )

        for b in range(33):
            for place, lanes in ((b, slice(0, 128)), (64 - b, slice(128, 256))):
                if b in (0, 32) and lanes.start:
                    continue
                low = code(products[16 * b : 16 * b + 8, lanes])
                top = code(products[16 * b + 8 : 16 * b + 16, lanes])
                words[8 * place : 8 * place + 8, :] = jnp.left_shift(top, 16) | (low & 0xFFFF)
        for p in range(4):
            tile = jnp.concatenate(
                [words[pl.ds(64 * g + i, 8, stride=8), :] for i in (2 * p, 2 * p + 1) for g in range(8)], 0
            )
            lanes = pl.ds(pl.multiple_of(512 * q + 128 * p, 128), 128)
            outbox[:, :, lanes] = tile.T.reshape(2, 64, 128)

        lanes = pl.ds(pl.multiple_of(512 * q, 512), 512)

        @pl.loop(0, 4)
        def _(k):
            for dy in range(4):
                place = wrap4(x + wrap4(k + dy)) * 8 + to_y[dy]
                for n, (add_t, add_row, to_col) in enumerate(corners):

                    def go(place=place, add_t=add_t, add_row=add_row, to_col=to_col):
                        pltpu.make_async_remote_copy(
                            outbox.at[:, pl.ds(place * 2 + add_t, 1), lanes],
                            inbox.at[:, pl.ds(me, 1), lanes],
                            s_out.at[q],
                            r_out.at[q],
                            **at(place + add_row, to_col),
                        ).start()

                    if dy == 0 and n == 0:
                        pl.when(k != 0)(go)
                    else:
                        go()

        pltpu.make_async_copy(
            outbox.at[:, pl.ds(me, 1), lanes], inbox.at[:, pl.ds(me, 1), lanes], r_out.at[q]
        ).start()

    def receive_phase(q):
        lanes = pl.ds(pl.multiple_of(512 * q, 512), 512)
        ref = inbox.at[:, :, lanes]
        pltpu.make_async_copy(ref, ref, r_out.at[q]).wait()
        for p in range(4):
            lanes = pl.ds(pl.multiple_of(512 * q + 128 * p, 128), 128)
            tile = inbox[:, :, lanes].reshape(128, 128).T
            rows = slice(128 * p, 128 * p + 128)
            low = decode(jnp.right_shift(jnp.left_shift(tile, 16), 16))
            b_hi[rows, 0:128], b_lo[rows, 0:128] = split(low)
            top = decode(jnp.right_shift(tile, 16))
            b_hi[rows, 128:256], b_lo[rows, 128:256] = split(top)
        high = b_hi[...]
        value = (
            jnp.dot(high, e_ref[0], preferred_element_type=F32)
            + jnp.dot(b_lo[...], e_ref[0], preferred_element_type=F32)
            + jnp.dot(high, e_ref[1], preferred_element_type=F32)
        )
        for i in range(8):
            re, im = value[64 * i : 64 * i + 64, 0:128], value[64 * i : 64 * i + 64, 128:256]
            cos = t2_ref[pl.ds(16 * q + 2 * i, 1), :]
            sin = t2_ref[pl.ds(16 * q + 2 * i + 1, 1), :]
            result[8 * q + i, :, 0:128] = re * cos - im * sin
            result[8 * q + i, :, 128:256] = re * sin + im * cos
        ref = pl.ds(8 * q, 8)
        pltpu.make_async_copy(result.at[ref], z_out.at[ref], z_sem.at[q]).start()

    @pl.loop(0, CHUNKS + LAG)
    def _(j):
        @pl.when(j == CHUNKS - 1)
        def _():
            pltpu.make_async_copy(last_in, last_in, r_last).wait()
            above[1:2, :] = above[0:1, :]
            above[0:1, :] = jnp.where(row * 2 + core == 0, jnp.zeros_like(last_in[...]), last_in[...])

        @pl.when(j == 2)
        def _():
            send_last()

        @pl.when(j < CHUNKS)
        def _():
            send_phase((j + 1) % CHUNKS)

        @pl.when(j >= LAG)
        def _():
            receive_phase((j - LAG + 1) % CHUNKS)

    for m in (1, 2, 3):
        pltpu.make_async_copy(edge.at[0], edge.at[0], s_edge).wait()
    for q in range(CHUNKS):
        ref = block.at[:, q, :, pl.ds(0, 6144)]
        pltpu.make_async_copy(ref, ref, s_blk.at[q]).wait()
        ref = outbox.at[0, pl.ds(0, 24), pl.ds(0, 2688)]
        pltpu.make_async_copy(ref, ref, s_out.at[q]).wait()
        ref = pl.ds(8 * q, 8)
        pltpu.make_async_copy(result.at[ref], z_out.at[ref], z_sem.at[q]).wait()
    for m in (1, 2, 3):
        pltpu.make_async_copy(last.at[0], last.at[0], s_last).wait()

    @pl.when(core == 0)
    def _():
        pltpu.make_async_copy(last.at[0], last.at[0], s_last).wait()


def run_exchange(mantissa, exponents):
    dma = pltpu.SemaphoreType.DMA
    operands = (
        mantissa.reshape(4, 8, 8, 2048),
        exponents,
        jnp.asarray(send_table()),
        jnp.asarray(receive_table()),
        jnp.asarray(np.concatenate([twist_table(33, 1.0), np.zeros((6, 128), np.float32)])),
        jnp.asarray(twist_table(64, DECODED / math.sqrt(NR * NC))),
    )
    return pl.pallas_call(
        exchange,
        out_shape=jax.ShapeDtypeStruct((64, 64, 256), F32),
        in_specs=[pl.BlockSpec(memory_space=pltpu.HBM)] * 6,
        out_specs=pl.BlockSpec(memory_space=pl.ANY),
        scratch_shapes=[
            pltpu.VMEM((2, 8, 8, 8192), BF16),
            pltpu.VMEM((64, 16, 128), F32),
            pltpu.VMEM((5, 8, 2, 16, 128), F32),
            pltpu.VMEM((528, 256), BF16),
            pltpu.VMEM((528, 256), BF16),
            pltpu.VMEM((528, 256), F32),
            pltpu.VMEM((512, 128), jnp.int32),
            pltpu.VMEM((2, 64, 4096), jnp.int32),
            pltpu.VMEM((2, 64, 4096), jnp.int32),
            pltpu.VMEM((512, 256), BF16),
            pltpu.VMEM((512, 256), BF16),
            pltpu.VMEM((64, 64, 256), F32),
            pltpu.SMEM((16, 64), jnp.int32),
            pltpu.VMEM((2, 256, 256), BF16),
            pltpu.VMEM((2, 256, 256), BF16),
            pltpu.VMEM((72, 128), F32),
            pltpu.VMEM((128, 128), F32),
            pltpu.VMEM((2, 4, 8, 2048), BF16),
            pltpu.VMEM((2, 2, 2048), F32),
            pltpu.VMEM((2, 8192), F32),
            pltpu.VMEM((2, 1, 2048), F32),
            pltpu.VMEM((1, 8192), F32),
            dma((CHUNKS,)),
            dma((CHUNKS,)),
            dma((CHUNKS,)),
            dma((CHUNKS,)),
            dma,
            dma,
            dma,
            dma,
            dma((4,)),
            dma((2,)),
            dma((CHUNKS,)),
            dma,
            pltpu.SemaphoreType.REGULAR,
            pltpu.SemaphoreType.REGULAR,
            pltpu.SemaphoreType.REGULAR,
        ],
        compiler_params=pltpu.CompilerParams(
            collective_id=0, has_side_effects=True, vmem_limit_bytes=48 * 1024 * 1024
        ),
        name="exchange",
    )(*[pltpu.with_memory_space_constraint(operand, pltpu.HBM) for operand in operands])


def finish(z_ref, re_ref, im_ref, middle):
    for i0 in range(8):
        spread = dft8([(z_ref[8 * i1 + i0, :, 0:128], z_ref[8 * i1 + i0, :, 128:256]) for i1 in range(8)])
        for k_a in range(8):
            value = twist64(spread[k_a], i0 * k_a)
            middle[k_a, i0, 0] = value[0]
            middle[k_a, i0, 1] = value[1]
    for k_a in range(8):
        spread = dft8([(middle[k_a, i0, 0], middle[k_a, i0, 1]) for i0 in range(8)])
        for k_b, (re, im) in enumerate(spread):
            lanes = slice(128 * (k_a + 8 * k_b), 128 * (k_a + 8 * k_b + 1))
            re_ref[:, lanes] = re
            im_ref[:, lanes] = im


def run_finish(z):
    return pl.pallas_call(
        finish,
        grid=(8,),
        out_shape=[jax.ShapeDtypeStruct((64, NR), F32)] * 2,
        in_specs=[pl.BlockSpec((64, 8, 256), lambda g: (0, g, 0))],
        out_specs=[pl.BlockSpec((8, NR), lambda g: (g, 0))] * 2,
        scratch_shapes=[pltpu.VMEM((8, 8, 2, 8, 128), F32)],
        compiler_params=pltpu.CompilerParams(vmem_limit_bytes=48 * 1024 * 1024),
        name="finish",
    )(z)


def local(mantissa, exponents):
    re, im = run_finish(run_exchange(mantissa, exponents))
    return re, im


def solution(mesh):
    in_specs = (P("rows", "cols"), P("rows", None))
    out_specs = (P(("rows", "cols"), None), P(("rows", "cols"), None))
    return jax.shard_map(local, mesh=mesh, in_specs=in_specs, out_specs=out_specs, check_vma=False)
```

```python
import math

import jax
import jax.numpy as jnp
import ml_dtypes
import numpy as np
from jax import lax
from jax.experimental import pallas as pl
from jax.experimental.pallas import tpu as pltpu
from jax.sharding import PartitionSpec as P

NR = 8192
NC = 8192
MESH = pl.DeviceIdType.MESH
CHUNKS = 8
LAG = 4
TOP = 32767.0
BOUND = 16896.0
DECODED = BOUND / TOP**4
F32 = jnp.float32
BF16 = jnp.bfloat16


def halves(table):
    high = table.astype(ml_dtypes.bfloat16)
    low = (table - high.astype(np.float64)).astype(ml_dtypes.bfloat16)
    return np.concatenate([high, high, low], 0)


def send_table():
    sides = []
    for side in range(2):
        t = np.arange(64)
        row, core = t // 2, t % 2
        z_lo = ((row // 4) % 2 + side) % 2
        a = 4 * row + 2 * z_lo + core
        jo = np.arange(128)[:, None]
        one = 2 * np.pi * (jo * a % 128) / 128
        two = 2 * np.pi * (jo * (a + 1) % 128) / 128
        from_re = np.concatenate([np.cos(one), -np.sin(one), np.cos(two), -np.sin(two)], 1)
        from_im = np.concatenate([np.sin(one), np.cos(one), -np.sin(two), -np.cos(two)], 1)
        sides.append(halves(np.concatenate([from_re, from_im], 0) / DECODED))
    return np.stack(sides)


def receive_table():
    k0 = np.arange(128)[None, :]
    blocks = []
    for half in range(2):
        s = 2 * np.arange(64)[:, None] + half
        angle = 2 * np.pi * (s * k0 % 128) / 128
        blocks.append(np.concatenate([np.cos(angle), -np.sin(angle)], 1))
        blocks.append(np.concatenate([np.sin(angle), np.cos(angle)], 1))
    return halves(np.concatenate(blocks, 0))


def twist_table(count, scale):
    angle = 2 * np.pi * (np.arange(count)[:, None] * np.arange(128)[None, :]) / 8192
    table = np.stack([np.cos(angle), -np.sin(angle)], 1).reshape(2 * count, 128) * scale
    return table.astype(np.float32)


def c_add(u, v):
    im = v[1] if u[1] is None else (u[1] if v[1] is None else u[1] + v[1])
    return (u[0] + v[0], im)


def c_sub(u, v):
    im = (None if v[1] is None else -v[1]) if u[1] is None else (u[1] if v[1] is None else u[1] - v[1])
    return (u[0] - v[0], im)


def sub_i(u, v):
    re = u[0] if v[1] is None else u[0] + v[1]
    return (re, -v[0] if u[1] is None else u[1] - v[0])


def add_i(u, v):
    re = u[0] if v[1] is None else u[0] - v[1]
    return (re, v[0] if u[1] is None else u[1] + v[0])


def c_scale(u, cos, sin):
    if u[1] is None:
        return (u[0] * cos, u[0] * (-sin))
    return (u[0] * cos + u[1] * sin, u[1] * cos - u[0] * sin)


ROOT = math.sqrt(0.5)


def dft4(x):
    t0, t1 = c_add(x[0], x[2]), c_sub(x[0], x[2])
    t2, t3 = c_add(x[1], x[3]), c_sub(x[1], x[3])
    return [c_add(t0, t2), sub_i(t1, t3), c_sub(t0, t2), add_i(t1, t3)]


def dft8(x, half=False):
    even, odd = dft4(x[0::2]), dft4(x[1::2])
    o1, o3 = odd[1], odd[3]
    w1 = ((o1[0] + o1[1]) * ROOT, (o1[1] - o1[0]) * ROOT)
    y = [c_add(even[0], odd[0]), c_add(even[1], w1), sub_i(even[2], odd[2]), None, c_sub(even[0], odd[0])]
    w3 = ((o3[1] - o3[0]) * ROOT, (o3[0] + o3[1]) * -ROOT)
    y[3] = c_add(even[3], w3)
    if half:
        return y
    return y + [c_sub(even[1], w1), add_i(even[2], odd[2]), c_sub(even[3], w3)]


def twist64(u, n):
    n = n % 64
    if n == 0:
        return u
    return c_scale(u, math.cos(2 * math.pi * n / 64), math.sin(2 * math.pi * n / 64))


def code(x):
    u = lax.rsqrt(lax.rsqrt(jnp.maximum(jnp.abs(x), 1e-12)))
    n = (u + 0.5).astype(jnp.int32)
    return jnp.where(x < 0, -n, n)


def decode(n):
    v = n.astype(F32)
    return (v * jnp.abs(v)) * (v * v)


def split(x):
    high = x.astype(BF16)
    return high, (x - high.astype(F32)).astype(BF16)


def exchange(
    mant, exps_in, send_w, recv_w, send_t, recv_t,
    z_out,
    block, masses, first, a_hi, a_lo, products, words, outbox, inbox, b_hi, b_lo, result,
    exps, scale_v, scales, w_ref, e_ref, t1_ref, t2_ref, edge_in, edge, above, last, last_in,
    s_blk, r_blk, s_out, r_out, s_edge, r_edge, s_last, r_last, tab_sem, edge_sem, z_sem, exp_sem, sem_b, sem_s, sem_c, sem_d,
):
    row, col = lax.axis_index("rows"), lax.axis_index("cols")
    x, z_hi, y = row // 8, (row // 4) % 2, row % 4
    z_lo, core = col // 2, col % 2
    side = (z_hi + z_lo) % 2
    me = row * 2 + core
    my_cols = pl.ds(pl.multiple_of(2048 * col, 2048), 2048)

    def at(r, c):
        return dict(device_id={"rows": r, "cols": c}, device_id_type=MESH)

    def wrap4(n):
        return jnp.where(n >= 4, n - 4, n)

    def mate(m):
        other = (core + m % 2) % 2
        return ((z_lo + m // 2) % 2) * 2 + other, other

    tables = (
        pltpu.make_async_copy(send_w.at[side], w_ref, tab_sem.at[0]),
        pltpu.make_async_copy(recv_w, e_ref, tab_sem.at[1]),
        pltpu.make_async_copy(send_t, t1_ref, tab_sem.at[2]),
        pltpu.make_async_copy(recv_t, t2_ref, tab_sem.at[3]),
    )
    edges = (
        pltpu.make_async_copy(mant.at[:, 0], edge_in.at[0], edge_sem.at[0]),
        pltpu.make_async_copy(mant.at[:, 7], edge_in.at[1], edge_sem.at[1]),
    )
    exp_copy = pltpu.make_async_copy(exps_in, exps, exp_sem.at[0])
    exp_copy.start()
    for copy in edges + tables:
        copy.start()

    barrier = pltpu.get_barrier_semaphore()
    away = at(x * 8 + (1 - z_hi) * 4 + y, (1 - z_lo) * 2 + core)
    sibling = at(row, z_lo * 2 + 1 - core)
    to_y = [wrap4(y + d) for d in range(4)]
    to_x = [wrap4(x + d) for d in range(4)]
    ring_x = [at(to_x[d] * 8 + z_hi * 4 + y, col) for d in (2, 1, 3)]
    ring_y = [at(x * 8 + z_hi * 4 + to_y[d], col) for d in (2, 1, 3)]
    group = [at(row, (1 - z_lo) * 2 + core), at(row, (1 - z_lo) * 2 + 1 - core), sibling]
    first_round = [away] + ring_x + ring_y + group
    for target in first_round:
        pl.semaphore_signal(barrier, inc=1, **target)

    exp_copy.wait()
    scale_v[...] = jnp.left_shift(1, exps[...] + 3).astype(F32) * 0.125
    scale_copy = pltpu.make_async_copy(scale_v, scales, exp_sem.at[1])
    scale_copy.start()
    scale_copy.wait()
    for copy in edges:
        copy.wait()
    for g in range(4):
        for j in range(16):
            lanes = slice(128 * j, 128 * (j + 1))
            scale = scales[4 * g, 16 * col + j]
            edge[g // 2, g % 2, :, lanes] = edge_in[0, g, :, lanes].astype(F32)[7:8] * scale
            if g % 2:
                scale = scales[4 * g + 3, 16 * col + j]
                last[g // 2, :, lanes] = edge_in[1, g, :, lanes].astype(F32)[7:8] * scale

    pl.semaphore_wait(barrier, len(first_round))
    for m in (1, 2, 3):
        c, other = mate(m)
        pltpu.make_async_remote_copy(
            edge.at[other], above.at[:, pl.ds(7, 1), my_cols], s_edge, r_edge, **at(row, c)
        ).start()
    pltpu.make_async_copy(edge.at[core], above.at[:, pl.ds(7, 1), my_cols], r_edge).start()

    def send_block(q):
        for c, other in (((1 - z_lo) * 2, 0), ((1 - z_lo) * 2 + 1, 1), (z_lo * 2 + 1 - core, 1 - core)):
            pltpu.make_async_remote_copy(
                mant.at[pl.ds(2 * other, 2), q], block.at[:, q, :, my_cols], s_blk.at[q], r_blk.at[q], **at(row, c)
            ).start()
        pltpu.make_async_copy(
            mant.at[pl.ds(2 * core, 2), q], block.at[:, q, :, my_cols], r_blk.at[q]
        ).start()

    send_block(1)
    for target in ring_y:
        pl.semaphore_signal(sem_b, inc=1, **target)

    @pl.loop(1, CHUNKS)
    def _(j):
        send_block((j + 1) % CHUNKS)

    pl.semaphore_wait(sem_b, 3)
    pl.semaphore_signal(sem_s, inc=1, **sibling)
    pl.semaphore_wait(sem_s, 1)
    pl.semaphore_signal(sem_c, inc=1, **away)

    for copy in tables:
        copy.wait()
    ref = above.at[:, pl.ds(7, 1)]
    pltpu.make_async_copy(ref, ref, r_edge).wait()
    sub8 = lax.broadcasted_iota(jnp.int32, (8, 128), 0)
    lane8 = lax.broadcasted_iota(jnp.int32, (8, 128), 1)

    def send_last():
        pl.semaphore_wait(sem_d, 1)
        for m in (1, 2, 3):
            c, other = mate(m)
            pltpu.make_async_remote_copy(
                last.at[1 - other], last_in.at[:, my_cols], s_last, r_last, **at((row + 1 - other) % 32, c)
            ).start()

        @pl.when(core == 1)
        def _():
            pltpu.make_async_copy(last.at[0], last_in.at[:, my_cols], r_last).start()

        @pl.when(core == 0)
        def _():
            pltpu.make_async_remote_copy(
                last.at[1], last_in.at[:, my_cols], s_last, r_last, **at((row + 1) % 32, col)
            ).start()

    corners = []
    for flip in range(2):
        for d in range(2):
            to_hi = 1 - z_hi if flip else z_hi
            to_lo = 1 - z_lo if flip else z_lo
            to_core = 1 - core if d else core
            corners.append((to_hi * 64 + to_core * 8, to_hi * 4, to_lo * 2 + to_core))

    def send_phase(q, j):
        ref = block.at[:, q]
        pltpu.make_async_copy(ref, ref, r_blk.at[q]).wait()

        for h in range(2):
            before = None
            for c in range(64):
                lanes = slice(128 * c, 128 * (c + 1))
                scale = scales[8 * core + 4 * h + q // 2, c]
                here = block[h, q, :, lanes].astype(F32) * scale
                top = jnp.broadcast_to(above[h, 7:8, lanes], (8, 128))
                upper = jnp.where(sub8 == 0, top, pltpu.roll(here, 1, 0))
                above[h, :, lanes] = here
                step = here - upper
                rolled = pltpu.roll(step, 1, 1)
                left = jnp.where(lane8 == 0, 0.0 if before is None else before, rolled)
                before = rolled
                masses[c, 8 * h : 8 * h + 8, :] = step - left

        for c0 in range(8):
            spread = dft8([(masses[8 * c1 + c0], None) for c1 in range(8)], half=True)
            for b1 in range(5):
                value = twist64(spread[b1], c0 * b1)
                first[b1, c0, 0] = value[0]
                if value[1] is not None:
                    first[b1, c0, 1] = value[1]
        for b1 in range(5):
            real = b1 == 0
            spread = dft8(
                [
                    (first[b1, c0, 0], None if real or (b1 == 4 and c0 == 0) else first[b1, c0, 1])
                    for c0 in range(8)
                ],
                half=real,
            )
            for b0, (re, im) in enumerate(spread):
                b = b1 + 8 * b0
                if b1 == 4 and b0 >= 4:
                    continue
                if b > 32:
                    b, im = 64 - b, -im
                if b == 0:
                    tw_re, tw_im = re, jnp.zeros_like(re)
                else:
                    cos = jnp.broadcast_to(t1_ref[2 * b : 2 * b + 1, :], (16, 128))
                    sin = jnp.broadcast_to(t1_ref[2 * b + 1 : 2 * b + 2, :], (16, 128))
                    if im is None:
                        tw_re, tw_im = re * cos, re * sin
                    else:
                        tw_re, tw_im = re * cos - im * sin, re * sin + im * cos
                rows = slice(16 * b, 16 * b + 16)
                a_hi[rows, 0:128], a_lo[rows, 0:128] = split(tw_re)
                a_hi[rows, 128:256], a_lo[rows, 128:256] = split(tw_im)

        high = a_hi[...]
        parts = jnp.concatenate([high, a_lo[...], high], 1)
        products[...] = jnp.dot(parts, w_ref[...], preferred_element_type=F32)

        for b in range(33):
            for place, lanes in ((b, slice(0, 128)), (64 - b, slice(128, 256))):
                if b in (0, 32) and lanes.start:
                    continue
                low = code(products[16 * b : 16 * b + 8, lanes])
                top = code(products[16 * b + 8 : 16 * b + 16, lanes])
                words[8 * place : 8 * place + 8, :] = jnp.left_shift(top, 16) | (low & 0xFFFF)
        start = pl.multiple_of(512 * q, 512)
        for p in range(4):
            tile = jnp.concatenate(
                [words[pl.ds(64 * g + i, 8, stride=8), :] for i in (2 * p, 2 * p + 1) for g in range(8)], 0
            )
            tile = tile.T
            for n in range(16):
                outbox[pl.ds(start + 64 * (n % 8) + 4 * (n // 8) + p, 8, stride=8), :] = tile[8 * n : 8 * n + 8]

        mine = pl.ds(pl.multiple_of(512 * q + 8 * me, 8), 8)

        for flip in range(2):
            if flip:

                @pl.when(j == 0)
                def _():
                    pl.semaphore_wait(sem_c, 1)
                    pl.semaphore_signal(sem_d, inc=1, **group[0])

            @pl.loop(0, 4)
            def _(k, flip=flip):
                for dy in range(4):
                    place = wrap4(x + wrap4(k + dy)) * 8 + to_y[dy]
                    for n, (add_t, add_row, to_col) in enumerate(corners[2 * flip : 2 * flip + 2]):
                        add_t = add_t + 512 * q

                        def go(place=place, add_t=add_t, add_row=add_row, to_col=to_col):
                            pltpu.make_async_remote_copy(
                                outbox.at[pl.ds(pl.multiple_of(place * 16 + add_t, 8), 8)],
                                inbox.at[mine],
                                s_out.at[q],
                                r_out.at[q],
                                **at(place + add_row, to_col),
                            ).start()

                        if flip == 0 and dy == 0 and n == 0:
                            pl.when(k != 0)(go)
                        else:
                            go()

        pltpu.make_async_copy(outbox.at[mine], inbox.at[mine], r_out.at[q]).start()

    def receive_phase(q):
        start = pl.multiple_of(512 * q, 512)
        ref = inbox.at[pl.ds(start, 512)]
        pltpu.make_async_copy(ref, ref, r_out.at[q]).wait()
        for p in range(4):
            tile = jnp.concatenate(
                [inbox[pl.ds(start + 64 * (n % 8) + 4 * (n // 8) + p, 8, stride=8), :] for n in range(16)], 0
            ).T
            rows = slice(128 * p, 128 * p + 128)
            low = decode(jnp.right_shift(jnp.left_shift(tile, 16), 16))
            b_hi[rows, 0:128], b_lo[rows, 0:128] = split(low)
            top = decode(jnp.right_shift(tile, 16))
            b_hi[rows, 128:256], b_lo[rows, 128:256] = split(top)
        high = b_hi[...]
        parts = jnp.concatenate([high, b_lo[...], high], 1)
        value = jnp.dot(parts, e_ref[...], preferred_element_type=F32)
        for i in range(8):
            re, im = value[64 * i : 64 * i + 64, 0:128], value[64 * i : 64 * i + 64, 128:256]
            cos = t2_ref[pl.ds(16 * q + 2 * i, 1), :]
            sin = t2_ref[pl.ds(16 * q + 2 * i + 1, 1), :]
            result[8 * q + i, :, 0:128] = re * cos - im * sin
            result[8 * q + i, :, 128:256] = re * sin + im * cos
        ref = pl.ds(8 * q, 8)
        pltpu.make_async_copy(result.at[ref], z_out.at[ref], z_sem.at[q]).start()

    @pl.loop(0, CHUNKS + LAG)
    def _(j):
        @pl.when(j == CHUNKS - 1)
        def _():
            pltpu.make_async_copy(last_in, last_in, r_last).wait()
            above[1, 7:8, :] = above[0, 7:8, :]
            above[0, 7:8, :] = jnp.where(row * 2 + core == 0, jnp.zeros_like(last_in[...]), last_in[...])

        @pl.when(j == 2)
        def _():
            send_last()

        @pl.when(j < CHUNKS)
        def _():
            send_phase((j + 1) % CHUNKS, j)

        @pl.when(j >= LAG)
        def _():
            receive_phase((j - LAG + 1) % CHUNKS)

    for m in (1, 2, 3):
        pltpu.make_async_copy(edge.at[0], edge.at[0], s_edge).wait()
    for q in range(CHUNKS):
        ref = block.at[:, q, :, pl.ds(0, 6144)]
        pltpu.make_async_copy(ref, ref, s_blk.at[q]).wait()
        ref = outbox.at[pl.ds(0, 504)]
        pltpu.make_async_copy(ref, ref, s_out.at[q]).wait()
        ref = pl.ds(8 * q, 8)
        pltpu.make_async_copy(result.at[ref], z_out.at[ref], z_sem.at[q]).wait()
    for m in (1, 2, 3):
        pltpu.make_async_copy(last.at[0], last.at[0], s_last).wait()

    @pl.when(core == 0)
    def _():
        pltpu.make_async_copy(last.at[0], last.at[0], s_last).wait()


def run_exchange(mantissa, exponents):
    dma = pltpu.SemaphoreType.DMA
    operands = (
        mantissa.reshape(4, 8, 8, 2048),
        exponents,
        jnp.asarray(send_table()),
        jnp.asarray(receive_table()),
        jnp.asarray(np.concatenate([twist_table(33, 1.0), np.zeros((6, 128), np.float32)])),
        jnp.asarray(twist_table(64, DECODED / math.sqrt(NR * NC))),
    )
    return pl.pallas_call(
        exchange,
        out_shape=jax.ShapeDtypeStruct((64, 64, 256), F32),
        in_specs=[pl.BlockSpec(memory_space=pltpu.HBM)] * 6,
        out_specs=pl.BlockSpec(memory_space=pl.ANY),
        scratch_shapes=[
            pltpu.VMEM((2, 8, 8, 8192), BF16),
            pltpu.VMEM((64, 16, 128), F32),
            pltpu.VMEM((5, 8, 2, 16, 128), F32),
            pltpu.VMEM((528, 256), BF16),
            pltpu.VMEM((528, 256), BF16),
            pltpu.VMEM((528, 256), F32),
            pltpu.VMEM((512, 128), jnp.int32),
            pltpu.VMEM((4096, 128), jnp.int32),
            pltpu.VMEM((4096, 128), jnp.int32),
            pltpu.VMEM((512, 256), BF16),
            pltpu.VMEM((512, 256), BF16),
            pltpu.VMEM((64, 64, 256), F32),
            pltpu.VMEM((16, 64), jnp.int32),
            pltpu.VMEM((16, 64), F32),
            pltpu.SMEM((16, 64), F32),
            pltpu.VMEM((768, 256), BF16),
            pltpu.VMEM((768, 256), BF16),
            pltpu.VMEM((72, 128), F32),
            pltpu.VMEM((128, 128), F32),
            pltpu.VMEM((2, 4, 8, 2048), BF16),
            pltpu.VMEM((2, 2, 1, 2048), F32),
            pltpu.VMEM((2, 8, 8192), F32),
            pltpu.VMEM((2, 1, 2048), F32),
            pltpu.VMEM((1, 8192), F32),
            dma((CHUNKS,)),
            dma((CHUNKS,)),
            dma((CHUNKS,)),
            dma((CHUNKS,)),
            dma,
            dma,
            dma,
            dma,
            dma((4,)),
            dma((2,)),
            dma((CHUNKS,)),
            dma((2,)),
            pltpu.SemaphoreType.REGULAR,
            pltpu.SemaphoreType.REGULAR,
            pltpu.SemaphoreType.REGULAR,
            pltpu.SemaphoreType.REGULAR,
        ],
        compiler_params=pltpu.CompilerParams(
            collective_id=0, has_side_effects=True, vmem_limit_bytes=48 * 1024 * 1024
        ),
        name="exchange",
    )(*[pltpu.with_memory_space_constraint(operand, pltpu.HBM) for operand in operands])


def finish(z_ref, re_out, im_out, re_ref, im_ref, middle, sems):
    def leave(g):
        rows = pl.ds(8 * g, 8)
        return (
            pltpu.make_async_copy(re_ref.at[rows], re_out.at[rows], sems.at[0, g]),
            pltpu.make_async_copy(im_ref.at[rows], im_out.at[rows], sems.at[1, g]),
        )

    @pl.loop(0, 8)
    def _(g):
        rows = pl.ds(pl.multiple_of(8 * g, 8), 8)
        for i0 in range(8):
            spread = dft8(
                [(z_ref[8 * i1 + i0, rows, 0:128], z_ref[8 * i1 + i0, rows, 128:256]) for i1 in range(8)]
            )
            for k_a in range(8):
                value = twist64(spread[k_a], i0 * k_a)
                middle[k_a, i0, 0] = value[0]
                middle[k_a, i0, 1] = value[1]
        for k_a in range(8):
            spread = dft8([(middle[k_a, i0, 0], middle[k_a, i0, 1]) for i0 in range(8)])
            for k_b, (re, im) in enumerate(spread):
                lanes = slice(128 * (k_a + 8 * k_b), 128 * (k_a + 8 * k_b + 1))
                re_ref[rows, lanes] = re
                im_ref[rows, lanes] = im
        for copy in leave(g):
            copy.start()

    for g in range(8):
        for copy in leave(g):
            copy.wait()


def run_finish(z):
    return pl.pallas_call(
        finish,
        out_shape=[jax.ShapeDtypeStruct((64, NR), F32)] * 2,
        in_specs=[pl.BlockSpec(memory_space=pltpu.VMEM)],
        out_specs=[pl.BlockSpec(memory_space=pl.ANY)] * 2,
        scratch_shapes=[
            pltpu.VMEM((64, NR), F32),
            pltpu.VMEM((64, NR), F32),
            pltpu.VMEM((8, 8, 2, 8, 128), F32),
            pltpu.SemaphoreType.DMA((2, 8)),
        ],
        compiler_params=pltpu.CompilerParams(vmem_limit_bytes=48 * 1024 * 1024),
        name="finish",
    )(z)


def local(mantissa, exponents):
    re, im = run_finish(run_exchange(mantissa, exponents))
    return re, im


def solution(mesh):
    in_specs = (P("rows", "cols"), P("rows", None))
    out_specs = (P(("rows", "cols"), None), P(("rows", "cols"), None))
    return jax.shard_map(local, mesh=mesh, in_specs=in_specs, out_specs=out_specs, check_vma=False)
```

```python
import math

import jax
import jax.numpy as jnp
import ml_dtypes
import numpy as np
from jax import lax
from jax.experimental import pallas as pl
from jax.experimental.pallas import tpu as pltpu
from jax.sharding import PartitionSpec as P

NR = 8192
NC = 8192
MESH = pl.DeviceIdType.MESH
CHUNKS = 8
LAG = 4
TOP = 32767.0
BOUND = 16896.0
DECODED = BOUND / TOP**4
F32 = jnp.float32
BF16 = jnp.bfloat16


def halves(table):
    high = table.astype(ml_dtypes.bfloat16)
    low = (table - high.astype(np.float64)).astype(ml_dtypes.bfloat16)
    return np.concatenate([high, high, low], 0)


def send_table():
    sides = []
    for side in range(2):
        t = np.arange(64)
        row, core = t // 2, t % 2
        z_lo = ((row // 4) % 2 + side) % 2
        a = 4 * row + 2 * z_lo + core
        jo = np.arange(128)[:, None]
        one = 2 * np.pi * (jo * a % 128) / 128
        two = 2 * np.pi * (jo * (a + 1) % 128) / 128
        from_re = np.concatenate([np.cos(one), -np.sin(one), np.cos(two), -np.sin(two)], 1)
        from_im = np.concatenate([np.sin(one), np.cos(one), -np.sin(two), -np.cos(two)], 1)
        sides.append(halves(np.concatenate([from_re, from_im], 0) / DECODED))
    return np.stack(sides)


def receive_table():
    k0 = np.arange(128)[None, :]
    blocks = []
    for half in range(2):
        s = 2 * np.arange(64)[:, None] + half
        angle = 2 * np.pi * (s * k0 % 128) / 128
        blocks.append(np.concatenate([np.cos(angle), -np.sin(angle)], 1))
        blocks.append(np.concatenate([np.sin(angle), np.cos(angle)], 1))
    return halves(np.concatenate(blocks, 0))


def twist_table(count, scale):
    angle = 2 * np.pi * (np.arange(count)[:, None] * np.arange(128)[None, :]) / 8192
    table = np.stack([np.cos(angle), -np.sin(angle)], 1).reshape(2 * count, 128) * scale
    return table.astype(np.float32)


def c_add(u, v):
    im = v[1] if u[1] is None else (u[1] if v[1] is None else u[1] + v[1])
    return (u[0] + v[0], im)


def c_sub(u, v):
    im = (None if v[1] is None else -v[1]) if u[1] is None else (u[1] if v[1] is None else u[1] - v[1])
    return (u[0] - v[0], im)


def sub_i(u, v):
    re = u[0] if v[1] is None else u[0] + v[1]
    return (re, -v[0] if u[1] is None else u[1] - v[0])


def add_i(u, v):
    re = u[0] if v[1] is None else u[0] - v[1]
    return (re, v[0] if u[1] is None else u[1] + v[0])


def c_scale(u, cos, sin):
    if u[1] is None:
        return (u[0] * cos, u[0] * (-sin))
    return (u[0] * cos + u[1] * sin, u[1] * cos - u[0] * sin)


ROOT = math.sqrt(0.5)


def dft4(x):
    t0, t1 = c_add(x[0], x[2]), c_sub(x[0], x[2])
    t2, t3 = c_add(x[1], x[3]), c_sub(x[1], x[3])
    return [c_add(t0, t2), sub_i(t1, t3), c_sub(t0, t2), add_i(t1, t3)]


def dft8(x, half=False):
    even, odd = dft4(x[0::2]), dft4(x[1::2])
    o1, o3 = odd[1], odd[3]
    w1 = ((o1[0] + o1[1]) * ROOT, (o1[1] - o1[0]) * ROOT)
    y = [c_add(even[0], odd[0]), c_add(even[1], w1), sub_i(even[2], odd[2]), None, c_sub(even[0], odd[0])]
    w3 = ((o3[1] - o3[0]) * ROOT, (o3[0] + o3[1]) * -ROOT)
    y[3] = c_add(even[3], w3)
    if half:
        return y
    return y + [c_sub(even[1], w1), add_i(even[2], odd[2]), c_sub(even[3], w3)]


def twist64(u, n):
    n = n % 64
    if n == 0:
        return u
    return c_scale(u, math.cos(2 * math.pi * n / 64), math.sin(2 * math.pi * n / 64))


def code(x):
    u = lax.rsqrt(lax.rsqrt(jnp.maximum(jnp.abs(x), 1e-12)))
    n = (u + 0.5).astype(jnp.int32)
    return jnp.where(x < 0, -n, n)


def decode(n):
    v = n.astype(F32)
    return (v * jnp.abs(v)) * (v * v)


def split(x):
    high = x.astype(BF16)
    return high, (x - high.astype(F32)).astype(BF16)


def exchange(
    mant, exps_in, send_w, recv_w, send_t, recv_t,
    z_out,
    block, masses, first, a_hi, a_lo, products, words, outbox, inbox, b_hi, b_lo,
    exps, scale_v, scales, w_ref, e_ref, t1_ref, t2_ref, edge_in, edge, edge_got, above, last, last_in,
    s_blk, r_blk, s_out, r_out, s_edge, r_edge, s_last, r_last, tab_sem, edge_sem, exp_sem, sem_b, sem_s, sem_c, sem_d,
):
    row, col = lax.axis_index("rows"), lax.axis_index("cols")
    x, z_hi, y = row // 8, (row // 4) % 2, row % 4
    z_lo, core = col // 2, col % 2
    side = (z_hi + z_lo) % 2
    me = row * 2 + core
    my_cols = pl.ds(pl.multiple_of(2048 * col, 2048), 2048)

    def at(r, c):
        return dict(device_id={"rows": r, "cols": c}, device_id_type=MESH)

    def wrap4(n):
        return jnp.where(n >= 4, n - 4, n)

    def mate(m):
        other = (core + m % 2) % 2
        return ((z_lo + m // 2) % 2) * 2 + other, other

    barrier = pltpu.get_barrier_semaphore()
    away = at(x * 8 + (1 - z_hi) * 4 + y, (1 - z_lo) * 2 + core)
    sibling = at(row, z_lo * 2 + 1 - core)
    to_y = [wrap4(y + d) for d in range(4)]
    to_x = [wrap4(x + d) for d in range(4)]
    ring_x = [at(to_x[d] * 8 + z_hi * 4 + y, col) for d in (2, 1, 3)]
    ring_y = [at(x * 8 + z_hi * 4 + to_y[d], col) for d in (2, 1, 3)]
    group = [at(row, (1 - z_lo) * 2 + core), at(row, (1 - z_lo) * 2 + 1 - core), sibling]
    first_round = [away] + ring_x + ring_y + group
    for target in first_round:
        pl.semaphore_signal(barrier, inc=1, **target)

    tables = (
        pltpu.make_async_copy(send_w.at[side], w_ref, tab_sem.at[0]),
        pltpu.make_async_copy(recv_w, e_ref, tab_sem.at[1]),
        pltpu.make_async_copy(send_t, t1_ref, tab_sem.at[2]),
        pltpu.make_async_copy(recv_t, t2_ref, tab_sem.at[3]),
    )
    edges = (
        pltpu.make_async_copy(mant.at[:, 0], edge_in.at[0], edge_sem.at[0]),
        pltpu.make_async_copy(mant.at[:, 7], edge_in.at[1], edge_sem.at[1]),
    )
    exp_copy = pltpu.make_async_copy(exps_in, exps, exp_sem.at[0])
    exp_copy.start()
    for copy in edges + tables:
        copy.start()

    exp_copy.wait()
    scale_v[...] = jnp.left_shift(1, exps[...] + 3).astype(F32) * 0.125
    scale_copy = pltpu.make_async_copy(scale_v, scales, exp_sem.at[1])
    scale_copy.start()
    scale_copy.wait()
    for copy in edges:
        copy.wait()
    for g in range(4):
        for j in range(16):
            lanes = slice(128 * j, 128 * (j + 1))
            scale = scales[4 * g, 16 * col + j]
            edge[g // 2, g % 2, :, lanes] = (edge_in[0, g, :, lanes].astype(F32)[7:8] * scale).astype(BF16)
            if g % 2:
                scale = scales[4 * g + 3, 16 * col + j]
                last[g // 2, :, lanes] = edge_in[1, g, :, lanes].astype(F32)[7:8] * scale

    pl.semaphore_wait(barrier, len(first_round))
    for m in (1, 2, 3):
        c, other = mate(m)
        pltpu.make_async_remote_copy(
            edge.at[other], edge_got.at[:, :, my_cols], s_edge, r_edge, **at(row, c)
        ).start()
    pltpu.make_async_copy(edge.at[core], edge_got.at[:, :, my_cols], r_edge).start()

    def send_block(q):
        for c, other in (((1 - z_lo) * 2, 0), ((1 - z_lo) * 2 + 1, 1), (z_lo * 2 + 1 - core, 1 - core)):
            pltpu.make_async_remote_copy(
                mant.at[pl.ds(2 * other, 2), q], block.at[:, q, :, my_cols], s_blk.at[q], r_blk.at[q], **at(row, c)
            ).start()
        pltpu.make_async_copy(
            mant.at[pl.ds(2 * core, 2), q], block.at[:, q, :, my_cols], r_blk.at[q]
        ).start()

    send_block(1)
    for target in ring_y:
        pl.semaphore_signal(sem_b, inc=1, **target)

    @pl.loop(1, CHUNKS)
    def _(j):
        send_block((j + 1) % CHUNKS)

    pl.semaphore_wait(sem_b, 3)
    pl.semaphore_signal(sem_s, inc=1, **sibling)
    pl.semaphore_wait(sem_s, 1)
    pl.semaphore_signal(sem_c, inc=1, **away)

    for copy in tables:
        copy.wait()
    pltpu.make_async_copy(edge_got, edge_got, r_edge).wait()
    for h in range(2):
        above[h, 7:8, :] = edge_got[h].astype(F32)
    sub8 = lax.broadcasted_iota(jnp.int32, (8, 128), 0)
    lane8 = lax.broadcasted_iota(jnp.int32, (8, 128), 1)

    def send_last():
        pl.semaphore_wait(sem_d, 1)
        for m in (1, 2, 3):
            c, other = mate(m)
            pltpu.make_async_remote_copy(
                last.at[1 - other], last_in.at[:, my_cols], s_last, r_last, **at((row + 1 - other) % 32, c)
            ).start()

        @pl.when(core == 1)
        def _():
            pltpu.make_async_copy(last.at[0], last_in.at[:, my_cols], r_last).start()

        @pl.when(core == 0)
        def _():
            pltpu.make_async_remote_copy(
                last.at[1], last_in.at[:, my_cols], s_last, r_last, **at((row + 1) % 32, col)
            ).start()

    hops = (0, 1, 2, 1)
    plane = sorted(((dx, dy) for dx in range(4) for dy in range(4)), key=lambda o: -hops[o[0]] - hops[o[1]])

    def send_phase(q, j):
        ref = block.at[:, q]
        pltpu.make_async_copy(ref, ref, r_blk.at[q]).wait()

        for h in range(2):
            before = None
            for c in range(64):
                lanes = slice(128 * c, 128 * (c + 1))
                scale = scales[8 * core + 4 * h + q // 2, c]
                here = block[h, q, :, lanes].astype(F32) * scale
                top = jnp.broadcast_to(above[h, 7:8, lanes], (8, 128))
                upper = jnp.where(sub8 == 0, top, pltpu.roll(here, 1, 0))
                above[h, :, lanes] = here
                step = here - upper
                rolled = pltpu.roll(step, 1, 1)
                left = jnp.where(lane8 == 0, 0.0 if before is None else before, rolled)
                before = rolled
                masses[c, 8 * h : 8 * h + 8, :] = step - left

        for c0 in range(8):
            spread = dft8([(masses[8 * c1 + c0], None) for c1 in range(8)], half=True)
            for b1 in range(5):
                value = twist64(spread[b1], c0 * b1)
                first[b1, c0, 0] = value[0]
                if value[1] is not None:
                    first[b1, c0, 1] = value[1]
        for b1 in range(5):
            real = b1 == 0
            spread = dft8(
                [
                    (first[b1, c0, 0], None if real or (b1 == 4 and c0 == 0) else first[b1, c0, 1])
                    for c0 in range(8)
                ],
                half=real,
            )
            for b0, (re, im) in enumerate(spread):
                b = b1 + 8 * b0
                if b1 == 4 and b0 >= 4:
                    continue
                if b > 32:
                    b, im = 64 - b, -im
                if b == 0:
                    tw_re, tw_im = re, jnp.zeros_like(re)
                else:
                    cos = jnp.broadcast_to(t1_ref[2 * b : 2 * b + 1, :], (16, 128))
                    sin = jnp.broadcast_to(t1_ref[2 * b + 1 : 2 * b + 2, :], (16, 128))
                    if im is None:
                        tw_re, tw_im = re * cos, re * sin
                    else:
                        tw_re, tw_im = re * cos - im * sin, re * sin + im * cos
                rows = slice(16 * b, 16 * b + 16)
                a_hi[rows, 0:128], a_lo[rows, 0:128] = split(tw_re)
                a_hi[rows, 128:256], a_lo[rows, 128:256] = split(tw_im)

        high = a_hi[...]
        parts = jnp.concatenate([high, a_lo[...], high], 1)
        products[...] = jnp.dot(parts, w_ref[...], preferred_element_type=F32)

        for b in range(33):
            for place, lanes in ((b, slice(0, 128)), (64 - b, slice(128, 256))):
                if b in (0, 32) and lanes.start:
                    continue
                low = code(products[16 * b : 16 * b + 8, lanes])
                top = code(products[16 * b + 8 : 16 * b + 16, lanes])
                words[8 * place : 8 * place + 8, :] = jnp.left_shift(top, 16) | (low & 0xFFFF)
        start = pl.multiple_of(512 * q, 512)
        for p in range(4):
            tile = jnp.concatenate(
                [words[pl.ds(64 * g + i, 8, stride=8), :] for i in (2 * p, 2 * p + 1) for g in range(8)], 0
            )
            tile = tile.T
            for n in range(16):
                outbox[pl.ds(start + 64 * (n % 8) + 4 * (n // 8) + p, 8, stride=8), :] = tile[8 * n : 8 * n + 8]

        mine = pl.ds(pl.multiple_of(512 * q + 8 * me, 8), 8)

        @pl.loop(0, 2)
        def _(turn):
            flip = turn

            @pl.when((j == 0) & (turn == 1))
            def _():
                pl.semaphore_wait(sem_c, 1)
                pl.semaphore_signal(sem_d, inc=1, **group[0])

            to_hi = jnp.where(flip == 1, 1 - z_hi, z_hi)
            to_lo = jnp.where(flip == 1, 1 - z_lo, z_lo)
            for dx, dy in plane:
                place = to_x[dx] * 8 + to_y[dy] + to_hi * 4
                for d in range(2):
                    to_core = 1 - core if d else core

                    def go(place=place, to_core=to_core):
                        pltpu.make_async_remote_copy(
                            outbox.at[pl.ds(pl.multiple_of(512 * q + place * 16 + to_core * 8, 8), 8)],
                            inbox.at[mine],
                            s_out.at[q],
                            r_out.at[q],
                            **at(place, to_lo * 2 + to_core),
                        ).start()

                    if (dx, dy, d) == (0, 0, 0):
                        pl.when(flip == 1)(go)
                    else:
                        go()

        pltpu.make_async_copy(outbox.at[mine], inbox.at[mine], r_out.at[q]).start()

    def receive_phase(q):
        start = pl.multiple_of(512 * q, 512)
        ref = inbox.at[pl.ds(start, 512)]
        pltpu.make_async_copy(ref, ref, r_out.at[q]).wait()
        for p in range(4):
            tile = jnp.concatenate(
                [inbox[pl.ds(start + 64 * (n % 8) + 4 * (n // 8) + p, 8, stride=8), :] for n in range(16)], 0
            ).T
            rows = slice(128 * p, 128 * p + 128)
            low = decode(jnp.right_shift(jnp.left_shift(tile, 16), 16))
            b_hi[rows, 0:128], b_lo[rows, 0:128] = split(low)
            top = decode(jnp.right_shift(tile, 16))
            b_hi[rows, 128:256], b_lo[rows, 128:256] = split(top)
        high = b_hi[...]
        parts = jnp.concatenate([high, b_lo[...], high], 1)
        value = jnp.dot(parts, e_ref[...], preferred_element_type=F32)
        for i in range(8):
            re, im = value[64 * i : 64 * i + 64, 0:128], value[64 * i : 64 * i + 64, 128:256]
            cos = t2_ref[pl.ds(16 * q + 2 * i, 1), :]
            sin = t2_ref[pl.ds(16 * q + 2 * i + 1, 1), :]
            z_out[8 * q + i, :, 0:128] = re * cos - im * sin
            z_out[8 * q + i, :, 128:256] = re * sin + im * cos

    @pl.loop(0, CHUNKS + LAG)
    def _(j):
        @pl.when(j == CHUNKS - 1)
        def _():
            pltpu.make_async_copy(last_in, last_in, r_last).wait()
            above[1, 7:8, :] = above[0, 7:8, :]
            above[0, 7:8, :] = jnp.where(row * 2 + core == 0, jnp.zeros_like(last_in[...]), last_in[...])

        @pl.when(j == 2)
        def _():
            send_last()

        @pl.when(j < CHUNKS)
        def _():
            send_phase((j + 1) % CHUNKS, j)

        @pl.when(j >= LAG)
        def _():
            receive_phase((j - LAG + 1) % CHUNKS)

    for m in (1, 2, 3):
        pltpu.make_async_copy(edge.at[0], edge.at[0], s_edge).wait()
    for q in range(CHUNKS):
        ref = block.at[:, q, :, pl.ds(0, 6144)]
        pltpu.make_async_copy(ref, ref, s_blk.at[q]).wait()
        ref = outbox.at[pl.ds(0, 504)]
        pltpu.make_async_copy(ref, ref, s_out.at[q]).wait()
    for m in (1, 2, 3):
        pltpu.make_async_copy(last.at[0], last.at[0], s_last).wait()

    @pl.when(core == 0)
    def _():
        pltpu.make_async_copy(last.at[0], last.at[0], s_last).wait()


def run_exchange(mantissa, exponents):
    dma = pltpu.SemaphoreType.DMA
    operands = (
        mantissa.reshape(4, 8, 8, 2048),
        exponents,
        jnp.asarray(send_table()),
        jnp.asarray(receive_table()),
        jnp.asarray(np.concatenate([twist_table(33, 1.0), np.zeros((6, 128), np.float32)])),
        jnp.asarray(twist_table(64, DECODED / math.sqrt(NR * NC))),
    )
    return pl.pallas_call(
        exchange,
        out_shape=jax.ShapeDtypeStruct((64, 64, 256), F32),
        in_specs=[pl.BlockSpec(memory_space=pltpu.HBM)] * 6,
        out_specs=pl.BlockSpec(memory_space=pltpu.VMEM),
        scratch_shapes=[
            pltpu.VMEM((2, 8, 8, 8192), BF16),
            pltpu.VMEM((64, 16, 128), F32),
            pltpu.VMEM((5, 8, 2, 16, 128), F32),
            pltpu.VMEM((528, 256), BF16),
            pltpu.VMEM((528, 256), BF16),
            pltpu.VMEM((528, 256), F32),
            pltpu.VMEM((512, 128), jnp.int32),
            pltpu.VMEM((4096, 128), jnp.int32),
            pltpu.VMEM((4096, 128), jnp.int32),
            pltpu.VMEM((512, 256), BF16),
            pltpu.VMEM((512, 256), BF16),
            pltpu.VMEM((16, 64), jnp.int32),
            pltpu.VMEM((16, 64), F32),
            pltpu.SMEM((16, 64), F32),
            pltpu.VMEM((768, 256), BF16),
            pltpu.VMEM((768, 256), BF16),
            pltpu.VMEM((72, 128), F32),
            pltpu.VMEM((128, 128), F32),
            pltpu.VMEM((2, 4, 8, 2048), BF16),
            pltpu.VMEM((2, 2, 1, 2048), BF16),
            pltpu.VMEM((2, 1, 8192), BF16),
            pltpu.VMEM((2, 8, 8192), F32),
            pltpu.VMEM((2, 1, 2048), F32),
            pltpu.VMEM((1, 8192), F32),
            dma((CHUNKS,)),
            dma((CHUNKS,)),
            dma((CHUNKS,)),
            dma((CHUNKS,)),
            dma,
            dma,
            dma,
            dma,
            dma((4,)),
            dma((2,)),
            dma((2,)),
            pltpu.SemaphoreType.REGULAR,
            pltpu.SemaphoreType.REGULAR,
            pltpu.SemaphoreType.REGULAR,
            pltpu.SemaphoreType.REGULAR,
        ],
        compiler_params=pltpu.CompilerParams(
            collective_id=0, has_side_effects=True, vmem_limit_bytes=48 * 1024 * 1024
        ),
        name="exchange",
    )(*[pltpu.with_memory_space_constraint(operand, pltpu.HBM) for operand in operands])


def finish(z_ref, re_out, im_out, re_ref, im_ref, middle, sems):
    def leave(g):
        rows = pl.ds(8 * g, 8)
        return (
            pltpu.make_async_copy(re_ref.at[rows], re_out.at[rows], sems.at[0, g]),
            pltpu.make_async_copy(im_ref.at[rows], im_out.at[rows], sems.at[1, g]),
        )

    @pl.loop(0, 8)
    def _(g):
        rows = pl.ds(pl.multiple_of(8 * g, 8), 8)
        for i0 in range(8):
            spread = dft8(
                [(z_ref[8 * i1 + i0, rows, 0:128], z_ref[8 * i1 + i0, rows, 128:256]) for i1 in range(8)]
            )
            for k_a in range(8):
                value = twist64(spread[k_a], i0 * k_a)
                middle[k_a, i0, 0] = value[0]
                middle[k_a, i0, 1] = value[1]
        for k_a in range(8):
            spread = dft8([(middle[k_a, i0, 0], middle[k_a, i0, 1]) for i0 in range(8)])
            for k_b, (re, im) in enumerate(spread):
                lanes = slice(128 * (k_a + 8 * k_b), 128 * (k_a + 8 * k_b + 1))
                re_ref[rows, lanes] = re
                im_ref[rows, lanes] = im
        for copy in leave(g):
            copy.start()

    for g in range(8):
        for copy in leave(g):
            copy.wait()


def run_finish(z):
    return pl.pallas_call(
        finish,
        out_shape=[jax.ShapeDtypeStruct((64, NR), F32)] * 2,
        in_specs=[pl.BlockSpec(memory_space=pltpu.VMEM)],
        out_specs=[pl.BlockSpec(memory_space=pl.ANY)] * 2,
        scratch_shapes=[
            pltpu.VMEM((64, NR), F32),
            pltpu.VMEM((64, NR), F32),
            pltpu.VMEM((8, 8, 2, 8, 128), F32),
            pltpu.SemaphoreType.DMA((2, 8)),
        ],
        compiler_params=pltpu.CompilerParams(vmem_limit_bytes=48 * 1024 * 1024),
        name="finish",
    )(z)


def local(mantissa, exponents):
    re, im = run_finish(run_exchange(mantissa, exponents))
    return re, im


def solution(mesh):
    in_specs = (P("rows", "cols"), P("rows", None))
    out_specs = (P(("rows", "cols"), None), P(("rows", "cols"), None))
    return jax.shard_map(local, mesh=mesh, in_specs=in_specs, out_specs=out_specs, check_vma=False)
```

```python
import math

import jax
import jax.numpy as jnp
import ml_dtypes
import numpy as np
from jax import lax
from jax.experimental import pallas as pl
from jax.experimental.pallas import tpu as pltpu
from jax.sharding import PartitionSpec as P

NR = 8192
NC = 8192
MESH = pl.DeviceIdType.MESH
CHUNKS = 8
LAG = 3
TOP = 32767.0
BOUND = 16896.0
DECODED = BOUND / TOP**4
F32 = jnp.float32
BF16 = jnp.bfloat16


def halves(table):
    high = table.astype(ml_dtypes.bfloat16)
    low = (table - high.astype(np.float64)).astype(ml_dtypes.bfloat16)
    return np.concatenate([high, high, low], 0)


def send_table():
    sides = []
    for side in range(2):
        t = np.arange(64)
        row, core = t // 2, t % 2
        z_lo = ((row // 4) % 2 + side) % 2
        a = 4 * row + 2 * z_lo + core
        jo = np.arange(128)[:, None]
        one = 2 * np.pi * (jo * a % 128) / 128
        two = 2 * np.pi * (jo * (a + 1) % 128) / 128
        from_re = np.concatenate([np.cos(one), -np.sin(one), np.cos(two), -np.sin(two)], 1)
        from_im = np.concatenate([np.sin(one), np.cos(one), -np.sin(two), -np.cos(two)], 1)
        sides.append(halves(np.concatenate([from_re, from_im], 0) / DECODED))
    return np.stack(sides)


def receive_table():
    k0 = np.arange(128)[None, :]
    blocks = []
    for half in range(2):
        s = 2 * np.arange(64)[:, None] + half
        angle = 2 * np.pi * (s * k0 % 128) / 128
        blocks.append(np.concatenate([np.cos(angle), -np.sin(angle)], 1))
        blocks.append(np.concatenate([np.sin(angle), np.cos(angle)], 1))
    return halves(np.concatenate(blocks, 0))


def twist_table(count, scale):
    angle = 2 * np.pi * (np.arange(count)[:, None] * np.arange(128)[None, :]) / 8192
    table = np.stack([np.cos(angle), -np.sin(angle)], 1).reshape(2 * count, 128) * scale
    return table.astype(np.float32)


def c_add(u, v):
    im = v[1] if u[1] is None else (u[1] if v[1] is None else u[1] + v[1])
    return (u[0] + v[0], im)


def c_sub(u, v):
    im = (None if v[1] is None else -v[1]) if u[1] is None else (u[1] if v[1] is None else u[1] - v[1])
    return (u[0] - v[0], im)


def sub_i(u, v):
    re = u[0] if v[1] is None else u[0] + v[1]
    return (re, -v[0] if u[1] is None else u[1] - v[0])


def add_i(u, v):
    re = u[0] if v[1] is None else u[0] - v[1]
    return (re, v[0] if u[1] is None else u[1] + v[0])


def c_scale(u, cos, sin):
    if u[1] is None:
        return (u[0] * cos, u[0] * (-sin))
    return (u[0] * cos + u[1] * sin, u[1] * cos - u[0] * sin)


ROOT = math.sqrt(0.5)


def dft4(x):
    t0, t1 = c_add(x[0], x[2]), c_sub(x[0], x[2])
    t2, t3 = c_add(x[1], x[3]), c_sub(x[1], x[3])
    return [c_add(t0, t2), sub_i(t1, t3), c_sub(t0, t2), add_i(t1, t3)]


def dft8(x, half=False):
    even, odd = dft4(x[0::2]), dft4(x[1::2])
    o1, o3 = odd[1], odd[3]
    w1 = ((o1[0] + o1[1]) * ROOT, (o1[1] - o1[0]) * ROOT)
    y = [c_add(even[0], odd[0]), c_add(even[1], w1), sub_i(even[2], odd[2]), None, c_sub(even[0], odd[0])]
    w3 = ((o3[1] - o3[0]) * ROOT, (o3[0] + o3[1]) * -ROOT)
    y[3] = c_add(even[3], w3)
    if half:
        return y
    return y + [c_sub(even[1], w1), add_i(even[2], odd[2]), c_sub(even[3], w3)]


def twist64(u, n):
    n = n % 64
    if n == 0:
        return u
    return c_scale(u, math.cos(2 * math.pi * n / 64), math.sin(2 * math.pi * n / 64))


def code(x):
    u = lax.rsqrt(lax.rsqrt(jnp.maximum(jnp.abs(x), 1e-12)))
    n = (u + 0.5).astype(jnp.int32)
    return jnp.where(x < 0, -n, n)


def decode(n):
    v = n.astype(F32)
    return (v * jnp.abs(v)) * (v * v)


def split(x):
    high = x.astype(BF16)
    return high, (x - high.astype(F32)).astype(BF16)


def exchange(
    mant, exps_in, send_w, recv_w, send_t, recv_t,
    z_out,
    block, masses, first, a_hi, a_lo, products, words, outbox, inbox, b_hi, b_lo,
    exps, scale_v, scales, w_ref, e_ref, t1_ref, t2_ref, edge_in, edge, edge_got, above, last, last_in,
    s_blk, r_blk, s_out, r_out, s_edge, r_edge, s_last, r_last, tab_sem, edge_sem, exp_sem, sem_b, sem_s, sem_c, sem_d,
):
    row, col = lax.axis_index("rows"), lax.axis_index("cols")
    x, z_hi, y = row // 8, (row // 4) % 2, row % 4
    z_lo, core = col // 2, col % 2
    side = (z_hi + z_lo) % 2
    me = row * 2 + core
    my_cols = pl.ds(pl.multiple_of(2048 * col, 2048), 2048)

    def at(r, c):
        return dict(device_id={"rows": r, "cols": c}, device_id_type=MESH)

    def wrap4(n):
        return jnp.where(n >= 4, n - 4, n)

    def mate(m):
        other = (core + m % 2) % 2
        return ((z_lo + m // 2) % 2) * 2 + other, other

    barrier = pltpu.get_barrier_semaphore()
    away = at(x * 8 + (1 - z_hi) * 4 + y, (1 - z_lo) * 2 + core)
    sibling = at(row, z_lo * 2 + 1 - core)
    to_y = [wrap4(y + d) for d in range(4)]
    to_x = [wrap4(x + d) for d in range(4)]
    ring_x = [at(to_x[d] * 8 + z_hi * 4 + y, col) for d in (2, 1, 3)]
    ring_y = [at(x * 8 + z_hi * 4 + to_y[d], col) for d in (2, 1, 3)]
    group = [at(row, (1 - z_lo) * 2 + core), at(row, (1 - z_lo) * 2 + 1 - core), sibling]
    first_round = [away] + ring_x + ring_y + group
    for target in first_round:
        pl.semaphore_signal(barrier, inc=1, **target)

    tables = (
        pltpu.make_async_copy(send_w.at[side], w_ref, tab_sem.at[0]),
        pltpu.make_async_copy(recv_w, e_ref, tab_sem.at[1]),
        pltpu.make_async_copy(send_t, t1_ref, tab_sem.at[2]),
        pltpu.make_async_copy(recv_t, t2_ref, tab_sem.at[3]),
    )
    edges = (
        pltpu.make_async_copy(mant.at[:, 0], edge_in.at[0], edge_sem.at[0]),
        pltpu.make_async_copy(mant.at[:, 7], edge_in.at[1], edge_sem.at[1]),
    )
    exp_copy = pltpu.make_async_copy(exps_in, exps, exp_sem.at[0])
    exp_copy.start()
    for copy in edges + tables:
        copy.start()

    exp_copy.wait()
    scale_v[...] = jnp.left_shift(1, exps[...] + 3).astype(F32) * 0.125
    scale_copy = pltpu.make_async_copy(scale_v, scales, exp_sem.at[1])
    scale_copy.start()
    scale_copy.wait()
    for copy in edges:
        copy.wait()
    for g in range(4):
        for j in range(16):
            lanes = slice(128 * j, 128 * (j + 1))
            scale = scales[4 * g, 16 * col + j]
            edge[g // 2, g % 2, :, lanes] = (edge_in[0, g, :, lanes].astype(F32)[7:8] * scale).astype(BF16)
            if g % 2:
                scale = scales[4 * g + 3, 16 * col + j]
                last[g // 2, :, lanes] = edge_in[1, g, :, lanes].astype(F32)[7:8] * scale

    pl.semaphore_wait(barrier, len(first_round))
    for m in (1, 2, 3):
        c, other = mate(m)
        pltpu.make_async_remote_copy(
            edge.at[other], edge_got.at[:, :, my_cols], s_edge, r_edge, **at(row, c)
        ).start()
    pltpu.make_async_copy(edge.at[core], edge_got.at[:, :, my_cols], r_edge).start()

    def send_block(q):
        for c, other in (((1 - z_lo) * 2, 0), ((1 - z_lo) * 2 + 1, 1), (z_lo * 2 + 1 - core, 1 - core)):
            pltpu.make_async_remote_copy(
                mant.at[pl.ds(2 * other, 2), q], block.at[:, q, :, my_cols], s_blk.at[q], r_blk.at[q], **at(row, c)
            ).start()
        pltpu.make_async_copy(
            mant.at[pl.ds(2 * core, 2), q], block.at[:, q, :, my_cols], r_blk.at[q]
        ).start()

    send_block(1)
    for target in ring_y:
        pl.semaphore_signal(sem_b, inc=1, **target)

    @pl.loop(1, CHUNKS)
    def _(j):
        send_block((j + 1) % CHUNKS)

    pl.semaphore_wait(sem_b, 3)
    pl.semaphore_signal(sem_s, inc=1, **sibling)
    pl.semaphore_wait(sem_s, 1)
    pl.semaphore_signal(sem_c, inc=1, **away)

    for copy in tables:
        copy.wait()
    pltpu.make_async_copy(edge_got, edge_got, r_edge).wait()
    for h in range(2):
        above[h, 7:8, :] = edge_got[h].astype(F32)
    sub8 = lax.broadcasted_iota(jnp.int32, (8, 128), 0)
    lane8 = lax.broadcasted_iota(jnp.int32, (8, 128), 1)

    def send_last():
        pl.semaphore_wait(sem_d, 1)
        for m in (1, 2, 3):
            c, other = mate(m)
            pltpu.make_async_remote_copy(
                last.at[1 - other], last_in.at[:, my_cols], s_last, r_last, **at((row + 1 - other) % 32, c)
            ).start()

        @pl.when(core == 1)
        def _():
            pltpu.make_async_copy(last.at[0], last_in.at[:, my_cols], r_last).start()

        @pl.when(core == 0)
        def _():
            pltpu.make_async_remote_copy(
                last.at[1], last_in.at[:, my_cols], s_last, r_last, **at((row + 1) % 32, col)
            ).start()

    hops = (0, 1, 2, 1)
    plane = sorted(((dx, dy) for dx in range(4) for dy in range(4)), key=lambda o: -hops[o[0]] - hops[o[1]])

    def send_phase(q, j):
        ref = block.at[:, q]
        pltpu.make_async_copy(ref, ref, r_blk.at[q]).wait()

        for h in range(2):
            before = None
            for c in range(64):
                lanes = slice(128 * c, 128 * (c + 1))
                scale = scales[8 * core + 4 * h + q // 2, c]
                here = block[h, q, :, lanes].astype(F32) * scale
                top = jnp.broadcast_to(above[h, 7:8, lanes], (8, 128))
                upper = jnp.where(sub8 == 0, top, pltpu.roll(here, 1, 0))
                above[h, :, lanes] = here
                step = here - upper
                rolled = pltpu.roll(step, 1, 1)
                left = jnp.where(lane8 == 0, 0.0 if before is None else before, rolled)
                before = rolled
                masses[c, 8 * h : 8 * h + 8, :] = step - left

        for c0 in range(8):
            spread = dft8([(masses[8 * c1 + c0], None) for c1 in range(8)], half=True)
            for b1 in range(5):
                value = twist64(spread[b1], c0 * b1)
                first[b1, c0, 0] = value[0]
                if value[1] is not None:
                    first[b1, c0, 1] = value[1]
        for b1 in range(5):
            real = b1 == 0
            spread = dft8(
                [
                    (first[b1, c0, 0], None if real or (b1 == 4 and c0 == 0) else first[b1, c0, 1])
                    for c0 in range(8)
                ],
                half=real,
            )
            for b0, (re, im) in enumerate(spread):
                b = b1 + 8 * b0
                if b1 == 4 and b0 >= 4:
                    continue
                if b > 32:
                    b, im = 64 - b, -im
                if b == 0:
                    tw_re, tw_im = re, jnp.zeros_like(re)
                else:
                    cos = jnp.broadcast_to(t1_ref[2 * b : 2 * b + 1, :], (16, 128))
                    sin = jnp.broadcast_to(t1_ref[2 * b + 1 : 2 * b + 2, :], (16, 128))
                    if im is None:
                        tw_re, tw_im = re * cos, re * sin
                    else:
                        tw_re, tw_im = re * cos - im * sin, re * sin + im * cos
                rows = slice(16 * b, 16 * b + 16)
                a_hi[rows, 0:128], a_lo[rows, 0:128] = split(tw_re)
                a_hi[rows, 128:256], a_lo[rows, 128:256] = split(tw_im)

        high = a_hi[...]
        parts = jnp.concatenate([high, a_lo[...], high], 1)
        products[...] = jnp.dot(parts, w_ref[...], preferred_element_type=F32)

        for b in range(33):
            for place, lanes in ((b, slice(0, 128)), (64 - b, slice(128, 256))):
                if b in (0, 32) and lanes.start:
                    continue
                low = code(products[16 * b : 16 * b + 8, lanes])
                top = code(products[16 * b + 8 : 16 * b + 16, lanes])
                words[8 * place : 8 * place + 8, :] = jnp.left_shift(top, 16) | (low & 0xFFFF)
        start = pl.multiple_of(512 * q, 512)
        for p in range(4):
            tile = jnp.concatenate(
                [words[pl.ds(64 * g + i, 8, stride=8), :] for i in (2 * p, 2 * p + 1) for g in range(8)], 0
            )
            tile = tile.T
            for n in range(16):
                outbox[pl.ds(start + 64 * (n % 8) + 4 * (n // 8) + p, 8, stride=8), :] = tile[8 * n : 8 * n + 8]

        mine = pl.ds(pl.multiple_of(512 * q + 8 * me, 8), 8)

        @pl.loop(0, 2)
        def _(turn):
            flip = turn

            @pl.when((j == 0) & (turn == 1))
            def _():
                pl.semaphore_wait(sem_c, 1)
                pl.semaphore_signal(sem_d, inc=1, **group[0])

            to_hi = jnp.where(flip == 1, 1 - z_hi, z_hi)
            to_lo = jnp.where(flip == 1, 1 - z_lo, z_lo)
            for dx, dy in plane:
                place = to_x[dx] * 8 + to_y[dy] + to_hi * 4
                for d in range(2):
                    to_core = 1 - core if d else core

                    def go(place=place, to_core=to_core):
                        pltpu.make_async_remote_copy(
                            outbox.at[pl.ds(pl.multiple_of(512 * q + place * 16 + to_core * 8, 8), 8)],
                            inbox.at[mine],
                            s_out.at[q],
                            r_out.at[q],
                            **at(place, to_lo * 2 + to_core),
                        ).start()

                    if (dx, dy, d) == (0, 0, 0):
                        pl.when(flip == 1)(go)
                    else:
                        go()

        pltpu.make_async_copy(outbox.at[mine], inbox.at[mine], r_out.at[q]).start()

    def receive_phase(q):
        start = pl.multiple_of(512 * q, 512)
        ref = inbox.at[pl.ds(start, 512)]
        pltpu.make_async_copy(ref, ref, r_out.at[q]).wait()
        for p in range(4):
            tile = jnp.concatenate(
                [inbox[pl.ds(start + 64 * (n % 8) + 4 * (n // 8) + p, 8, stride=8), :] for n in range(16)], 0
            ).T
            rows = slice(128 * p, 128 * p + 128)
            low = decode(jnp.right_shift(jnp.left_shift(tile, 16), 16))
            b_hi[rows, 0:128], b_lo[rows, 0:128] = split(low)
            top = decode(jnp.right_shift(tile, 16))
            b_hi[rows, 128:256], b_lo[rows, 128:256] = split(top)
        high = b_hi[...]
        parts = jnp.concatenate([high, b_lo[...], high], 1)
        value = jnp.dot(parts, e_ref[...], preferred_element_type=F32)
        for i in range(8):
            re, im = value[64 * i : 64 * i + 64, 0:128], value[64 * i : 64 * i + 64, 128:256]
            cos = t2_ref[pl.ds(16 * q + 2 * i, 1), :]
            sin = t2_ref[pl.ds(16 * q + 2 * i + 1, 1), :]
            z_out[8 * q + i, :, 0:128] = re * cos - im * sin
            z_out[8 * q + i, :, 128:256] = re * sin + im * cos

    @pl.loop(0, CHUNKS + LAG)
    def _(j):
        @pl.when(j == CHUNKS - 1)
        def _():
            pltpu.make_async_copy(last_in, last_in, r_last).wait()
            above[1, 7:8, :] = above[0, 7:8, :]
            above[0, 7:8, :] = jnp.where(row * 2 + core == 0, jnp.zeros_like(last_in[...]), last_in[...])

        @pl.when(j == 2)
        def _():
            send_last()

        @pl.when(j < CHUNKS)
        def _():
            send_phase((j + 1) % CHUNKS, j)

        @pl.when(j >= LAG)
        def _():
            receive_phase((j - LAG + 1) % CHUNKS)

    for m in (1, 2, 3):
        pltpu.make_async_copy(edge.at[0], edge.at[0], s_edge).wait()
    for q in range(CHUNKS):
        ref = block.at[:, q, :, pl.ds(0, 6144)]
        pltpu.make_async_copy(ref, ref, s_blk.at[q]).wait()
        ref = outbox.at[pl.ds(0, 504)]
        pltpu.make_async_copy(ref, ref, s_out.at[q]).wait()
    for m in (1, 2, 3):
        pltpu.make_async_copy(last.at[0], last.at[0], s_last).wait()

    @pl.when(core == 0)
    def _():
        pltpu.make_async_copy(last.at[0], last.at[0], s_last).wait()


def run_exchange(mantissa, exponents):
    dma = pltpu.SemaphoreType.DMA
    operands = (
        mantissa.reshape(4, 8, 8, 2048),
        exponents,
        jnp.asarray(send_table()),
        jnp.asarray(receive_table()),
        jnp.asarray(np.concatenate([twist_table(33, 1.0), np.zeros((6, 128), np.float32)])),
        jnp.asarray(twist_table(64, DECODED / math.sqrt(NR * NC))),
    )
    return pl.pallas_call(
        exchange,
        out_shape=jax.ShapeDtypeStruct((64, 64, 256), F32),
        in_specs=[pl.BlockSpec(memory_space=pltpu.HBM)] * 6,
        out_specs=pl.BlockSpec(memory_space=pltpu.VMEM),
        scratch_shapes=[
            pltpu.VMEM((2, 8, 8, 8192), BF16),
            pltpu.VMEM((64, 16, 128), F32),
            pltpu.VMEM((5, 8, 2, 16, 128), F32),
            pltpu.VMEM((528, 256), BF16),
            pltpu.VMEM((528, 256), BF16),
            pltpu.VMEM((528, 256), F32),
            pltpu.VMEM((512, 128), jnp.int32),
            pltpu.VMEM((4096, 128), jnp.int32),
            pltpu.VMEM((4096, 128), jnp.int32),
            pltpu.VMEM((512, 256), BF16),
            pltpu.VMEM((512, 256), BF16),
            pltpu.VMEM((16, 64), jnp.int32),
            pltpu.VMEM((16, 64), F32),
            pltpu.SMEM((16, 64), F32),
            pltpu.VMEM((768, 256), BF16),
            pltpu.VMEM((768, 256), BF16),
            pltpu.VMEM((72, 128), F32),
            pltpu.VMEM((128, 128), F32),
            pltpu.VMEM((2, 4, 8, 2048), BF16),
            pltpu.VMEM((2, 2, 1, 2048), BF16),
            pltpu.VMEM((2, 1, 8192), BF16),
            pltpu.VMEM((2, 8, 8192), F32),
            pltpu.VMEM((2, 1, 2048), F32),
            pltpu.VMEM((1, 8192), F32),
            dma((CHUNKS,)),
            dma((CHUNKS,)),
            dma((CHUNKS,)),
            dma((CHUNKS,)),
            dma,
            dma,
            dma,
            dma,
            dma((4,)),
            dma((2,)),
            dma((2,)),
            pltpu.SemaphoreType.REGULAR,
            pltpu.SemaphoreType.REGULAR,
            pltpu.SemaphoreType.REGULAR,
            pltpu.SemaphoreType.REGULAR,
        ],
        compiler_params=pltpu.CompilerParams(
            collective_id=0, has_side_effects=True, vmem_limit_bytes=48 * 1024 * 1024
        ),
        name="exchange",
    )(*[pltpu.with_memory_space_constraint(operand, pltpu.HBM) for operand in operands])


def finish(z_ref, re_out, im_out, re_ref, im_ref, middle, sems):
    def leave(g):
        rows = pl.ds(8 * g, 8)
        return (
            pltpu.make_async_copy(re_ref.at[rows], re_out.at[rows], sems.at[0, g]),
            pltpu.make_async_copy(im_ref.at[rows], im_out.at[rows], sems.at[1, g]),
        )

    @pl.loop(0, 8)
    def _(g):
        rows = pl.ds(pl.multiple_of(8 * g, 8), 8)
        for i0 in range(8):
            spread = dft8(
                [(z_ref[8 * i1 + i0, rows, 0:128], z_ref[8 * i1 + i0, rows, 128:256]) for i1 in range(8)]
            )
            for k_a in range(8):
                value = twist64(spread[k_a], i0 * k_a)
                middle[k_a, i0, 0] = value[0]
                middle[k_a, i0, 1] = value[1]
        for k_a in range(8):
            spread = dft8([(middle[k_a, i0, 0], middle[k_a, i0, 1]) for i0 in range(8)])
            for k_b, (re, im) in enumerate(spread):
                lanes = slice(128 * (k_a + 8 * k_b), 128 * (k_a + 8 * k_b + 1))
                re_ref[rows, lanes] = re
                im_ref[rows, lanes] = im
        for copy in leave(g):
            copy.start()

    for g in range(8):
        for copy in leave(g):
            copy.wait()


def run_finish(z):
    return pl.pallas_call(
        finish,
        out_shape=[jax.ShapeDtypeStruct((64, NR), F32)] * 2,
        in_specs=[pl.BlockSpec(memory_space=pltpu.VMEM)],
        out_specs=[pl.BlockSpec(memory_space=pl.ANY)] * 2,
        scratch_shapes=[
            pltpu.VMEM((64, NR), F32),
            pltpu.VMEM((64, NR), F32),
            pltpu.VMEM((8, 8, 2, 8, 128), F32),
            pltpu.SemaphoreType.DMA((2, 8)),
        ],
        compiler_params=pltpu.CompilerParams(vmem_limit_bytes=48 * 1024 * 1024),
        name="finish",
    )(z)


def local(mantissa, exponents):
    re, im = run_finish(run_exchange(mantissa, exponents))
    return re, im


def solution(mesh):
    in_specs = (P("rows", "cols"), P("rows", None))
    out_specs = (P(("rows", "cols"), None), P(("rows", "cols"), None))
    return jax.shard_map(local, mesh=mesh, in_specs=in_specs, out_specs=out_specs, check_vma=False)
```
